128 devices in a mesh: seq: 8 (over y, core), span: 16 (over x, z).
Axes of the slice: x: 4, y: 4, z: 4, core: 2. Of those that a mesh axis runs over, the one named last changes fastest.
Arguments:
- queries: bfloat16 [16, 1024, 1536], P('span', 'seq'), may hold values from -6 to 6
- key_head_matrix: bfloat16 [16, 1024, 512], P('span', 'seq'), may hold values from -6 to 6
- value_head_matrix: bfloat16 [16, 1024, 512], P('span', 'seq'), may hold values from -6 to 6
- attn_output: bfloat16 [16, 1024, 1536], P('span', 'seq'), may hold values from -6 to 6
- out_grad: bfloat16 [16, 1024, 1536], P('span', 'seq'), may hold values from -6 to 6
Outputs:
- query_grad: bfloat16 [16, 1024, 1536], P('span', 'seq')
- key_grad: bfloat16 [16, 1024, 512], P('span', 'seq')
- value_grad: bfloat16 [16, 1024, 512], P('span', 'seq')
The draws below stay inside these ranges and needn't reach their ends.
All inputs are finite; a program needn't handle non-finite values.
Results may differ from the reference program's by a relative error of at most 0.005.
Values may be sent and summed in bfloat16 or wider, within the bound.
A program may use at most 64 MiB of HBM per device.

```python
import math
import jax
import jax.numpy as jnp
from jax import lax

HEAD_WIDTH = 64
KEY_HEADS = 8
QUERY_PER_KEY = 3
HQ = 24
BLOCK_TOKENS = 1024
SEQUENCE_BLOCKS = 16


def draw_queries(key, part):
    random_seed_key = jax.random.fold_in(key, 1)
    value_rows = jax.random.truncated_normal(random_seed_key, -6.0, 6.0, (SEQUENCE_BLOCKS, BLOCK_TOKENS, HQ * HEAD_WIDTH), jnp.float32)
    return value_rows.astype(jnp.bfloat16)


def draw_key_head_matrix(key, part):
    random_seed_key = jax.random.fold_in(key, 2)
    value_rows = jax.random.truncated_normal(random_seed_key, -6.0, 6.0, (SEQUENCE_BLOCKS, BLOCK_TOKENS, KEY_HEADS * HEAD_WIDTH), jnp.float32)
    return value_rows.astype(jnp.bfloat16)


def shard_levels(own_key, shape, split, smallest, largest):
    gain = 1.0
    for position, blocks in split:
        heights = jax.random.uniform(jax.random.fold_in(jax.random.fold_in(own_key, 6), position), (blocks,), jnp.float32, smallest / len(split), largest / len(split))
        gain = gain * jnp.repeat(jnp.exp(heights), shape[position] // blocks).reshape((-1,) + (1,) * (len(shape) - 1 - position))
    return gain


def bell_draw(own_key, extent, scale, limit, split=(), held_as=jnp.bfloat16):
    values = jax.random.normal(own_key, extent, jnp.float32) * scale
    if len(split) > 0:
        values = shard_levels(own_key, extent, split, -0.22, 0.18) * values
    return jnp.clip(values, min=-limit, max=limit).astype(held_as)


def setup_inputs(seed: int = 0) -> dict:
    key_of = jax.random.split(jax.random.key(seed), 6)
    queries = draw_queries(jax.random.fold_in(key_of[5], 71), 0)
    key_head_matrix = draw_key_head_matrix(jax.random.fold_in(key_of[5], 71), 0)
    value_head_matrix = bell_draw(key_of[2], (SEQUENCE_BLOCKS, BLOCK_TOKENS, KEY_HEADS * HEAD_WIDTH), 1.0, 6.0, ((0, 16), (1, 8)))
    attn_output = bell_draw(key_of[3], (SEQUENCE_BLOCKS, BLOCK_TOKENS, HQ * HEAD_WIDTH), 1.0, 6.0, ((0, 16), (1, 8)))
    out_grad = bell_draw(key_of[4], (SEQUENCE_BLOCKS, BLOCK_TOKENS, HQ * HEAD_WIDTH), 1.0, 6.0, ((0, 16), (1, 8)))
    return {"queries": queries, "key_head_matrix": key_head_matrix, "value_head_matrix": value_head_matrix, "attn_output": attn_output, "out_grad": out_grad}


NEG_LARGE = -1e+30

def head_grads(running, inputs):
    query_head, key_head, value_head, output_head, grad_head = inputs
    sequence_length = query_head.shape[0]
    scaling = 1.0 / math.sqrt(HEAD_WIDTH)
    positions = lax.iota(jnp.int32, sequence_length)
    allowed = positions[None, :] <= positions[:, None]
    scores = jnp.dot(query_head, key_head.T, preferred_element_type=jnp.float32) * scaling
    row_max = lax.optimization_barrier(jnp.max(jnp.where(allowed, scores, NEG_LARGE), axis=1))
    row_sum = lax.optimization_barrier(jnp.sum(jnp.where(allowed, jnp.exp(scores - row_max[:, None]), 0.0), axis=1))
    log_norm = row_max + jnp.log(row_sum)
    prob_weights = jnp.where(allowed, jnp.exp(scores - log_norm[:, None]), 0.0)
    row_delta = lax.optimization_barrier(jnp.sum(grad_head.astype(jnp.float32) * output_head.astype(jnp.float32), axis=1))
    prob_grad = jnp.dot(grad_head, value_head.T, preferred_element_type=jnp.float32)
    score_low = (prob_weights * (prob_grad - row_delta[:, None])).astype(jnp.bfloat16)
    prob_low = prob_weights.astype(jnp.bfloat16)
    query_part = scaling * jnp.dot(score_low, key_head, preferred_element_type=jnp.float32)
    key_piece = scaling * jnp.dot(score_low.T, query_head, preferred_element_type=jnp.float32)
    value_piece = jnp.dot(prob_low.T, grad_head, preferred_element_type=jnp.float32)
    return (running, (query_part, key_piece, value_piece))

def reference(queries, key_head_matrix, value_head_matrix, attn_output, out_grad):
    sequence_length = SEQUENCE_BLOCKS * BLOCK_TOKENS

    def each_head_share(source, head_count):
        return jnp.transpose(source.reshape(sequence_length, head_count, HEAD_WIDTH), (1, 0, 2))
    key_complete = jnp.repeat(each_head_share(key_head_matrix, KEY_HEADS), QUERY_PER_KEY, axis=0)
    value_complete = jnp.repeat(each_head_share(value_head_matrix, KEY_HEADS), QUERY_PER_KEY, axis=0)
    start_state = jnp.zeros((), jnp.float32)
    final_state, head_results = lax.scan(head_grads, start_state, (each_head_share(queries, HQ), key_complete, value_complete, each_head_share(attn_output, HQ), each_head_share(out_grad, HQ)))
    query_part, key_piece, value_piece = head_results
    query_out = jnp.transpose(query_part, (1, 0, 2)).reshape(SEQUENCE_BLOCKS, BLOCK_TOKENS, HQ * HEAD_WIDTH).astype(jnp.bfloat16)
    key_total = lax.optimization_barrier(jnp.sum(key_piece.reshape(KEY_HEADS, QUERY_PER_KEY, sequence_length, HEAD_WIDTH), axis=1))
    value_total = lax.optimization_barrier(jnp.sum(value_piece.reshape(KEY_HEADS, QUERY_PER_KEY, sequence_length, HEAD_WIDTH), axis=1))
    key_result = jnp.transpose(key_total, (1, 0, 2)).reshape(SEQUENCE_BLOCKS, BLOCK_TOKENS, KEY_HEADS * HEAD_WIDTH).astype(jnp.bfloat16)
    value_result = jnp.transpose(value_total, (1, 0, 2)).reshape(SEQUENCE_BLOCKS, BLOCK_TOKENS, KEY_HEADS * HEAD_WIDTH).astype(jnp.bfloat16)
    return (query_out, key_result, value_result)
```

```python
import functools
import math

import jax
import jax.numpy as jnp
from jax import lax
from jax.experimental import pallas as pl
from jax.experimental.pallas import tpu as pltpu
from jax.sharding import PartitionSpec as P

HEAD_WIDTH = 64
QUERY_PER_KEY = 3
TILE = 512
CHUNK = 256
LANES = 128
NEG_LARGE = -1e30
SCORE_SCALE = 1.0 / math.sqrt(HEAD_WIDTH)
BASE2_SCALE = SCORE_SCALE * math.log2(math.e)
F32 = jnp.float32
BF16 = jnp.bfloat16


def dot(a, b, contract):
    return lax.dot_general(a, b, ((contract[0], contract[1]), ((), ())), preferred_element_type=F32)


def three_parts(x):
    first = x.astype(BF16).astype(F32)
    rest = x - first
    second = rest.astype(BF16).astype(F32)
    return first, second, rest - second


def compute_kernel(spans, qdo_ref, delta_ref, kv_ref, dq_ref, dkv_ref, lt, l2, ks1, ks2, vs1, stat_m, stat_l, dq_acc, p_buf, ds_buf):
    own = lax.axis_index("span")
    rows = QUERY_PER_KEY * TILE
    key_tiles = kv_ref.shape[0] // TILE
    diag = (2 * own, key_tiles - 1 - 2 * own)
    lane = lax.broadcasted_iota(jnp.int32, (TILE, LANES), 1)
    aux_s = jnp.where((lane >= 64) & (lane < 67), -1.0, 0.0)
    aux_v = jnp.where((lane >= 67) & (lane < 70), -1.0, 0.0).astype(BF16)

    @pl.loop(0, key_tiles)
    def _(t):
        at = pl.ds(pl.multiple_of(t * TILE, TILE), TILE)
        raw = kv_ref[at, :].astype(F32)
        scaled = raw * BASE2_SCALE
        high = scaled.astype(BF16).astype(F32)
        ks1[at, :] = jnp.where(lane < 64, high, 0.0).astype(BF16)
        ks2[at, :] = jnp.where(lane < 64, scaled - high, aux_s).astype(BF16)
        vs1[at, :] = jnp.where(lane >= 64, raw, 0.0).astype(BF16)
        dkv_ref[:, at] = jnp.zeros((LANES, TILE), F32)

    for u in range(2):
        for h in range(QUERY_PER_KEY):
            cols = pl.ds(h * TILE, TILE)
            turned = qdo_ref[u, h].astype(F32).T
            lt[u, 0:128, cols] = turned.astype(BF16)
            lt[u, 128:256, cols] = jnp.concatenate([turned[0:64], jnp.zeros((64, TILE), F32)], axis=0).astype(BF16)
        dq_acc[u] = jnp.zeros((rows, LANES), F32)
        stat_m[u] = jnp.full((8, rows), NEG_LARGE, F32)
        stat_l[u] = jnp.zeros((8, rows), F32)

    key_at = lax.broadcasted_iota(jnp.int32, (TILE, TILE), 0)
    query_at = lax.broadcasted_iota(jnp.int32, (TILE, TILE), 1)

    def stats(u, t, masked):
        at = pl.ds(pl.multiple_of(t * TILE, TILE), TILE)
        w = jnp.concatenate([ks1[at, :], ks2[at, :]], axis=1)
        for h in range(QUERY_PER_KEY):
            cols = pl.ds(h * TILE, TILE)
            s = dot(w, lt[u, :, cols], ((1,), (0,)))
            if masked:
                s = jnp.where(key_at <= query_at, s, NEG_LARGE)
            old = stat_m[u, 0:1, cols]
            new = jnp.maximum(old, jnp.max(s, axis=0, keepdims=True))
            e = jnp.exp2(s - new)
            part = jnp.sum(e.reshape(TILE // 8, 8, TILE), axis=0)
            stat_l[u, :, cols] = stat_l[u, :, cols] * jnp.exp2(old - new) + part
            stat_m[u, :, cols] = jnp.broadcast_to(new, (8, TILE))

    for u in range(2):
        @pl.loop(0, diag[u])
        def _(t):
            stats(u, t, False)

        stats(u, diag[u], True)

    row = lax.broadcasted_iota(jnp.int32, (16, TILE), 0)
    for u in range(2):
        for h in range(QUERY_PER_KEY):
            cols = pl.ds(h * TILE, TILE)
            total = jnp.sum(stat_l[u, :, cols], axis=0, keepdims=True)
            lse = stat_m[u, 0:1, cols] + jnp.log2(total)
            parts = three_parts(lse) + three_parts(delta_ref[u, h : h + 1, :])
            block = jnp.zeros((16, TILE), F32)
            for i, part in enumerate(parts):
                block = jnp.where(row == i, part, block)
            lt[u, 192:208, cols] = block.astype(BF16)
            l2[u, h] = lt[u, 128:256, cols].astype(F32).T.astype(BF16)

    def main(u, t, masked):
        at = pl.ds(pl.multiple_of(t * TILE, TILE), TILE)
        kw = jnp.concatenate([ks1[at, :], ks2[at, :]], axis=1)
        vw = jnp.concatenate([vs1[at, :], aux_v], axis=1)
        kv = kv_ref[at, :]
        if masked:
            key_col = lax.broadcasted_iota(jnp.int32, (CHUNK, TILE), 1)
            query_row = lax.broadcasted_iota(jnp.int32, (CHUNK, TILE), 0)
        for h in range(QUERY_PER_KEY):
            for first in range(0, TILE, CHUNK):
                here = pl.ds(h * TILE + first, CHUNK)
                lhs = jnp.concatenate([qdo_ref[u, h, first : first + CHUNK, :], l2[u, h, first : first + CHUNK, :]], axis=1)
                s = dot(lhs, kw, ((1,), (1,)))
                dp = dot(lhs, vw, ((1,), (1,)))
                p = jnp.exp2(s)
                if masked:
                    p = jnp.where(key_col <= query_row + first, p, 0.0)
                ds = (p * dp).astype(BF16)
                p_buf[here, :] = p.astype(BF16)
                ds_buf[here, :] = ds
                dq_acc[u, here, :] += dot(ds, kv, ((1,), (0,)))
        dkv_ref[0:64, at] += dot(lt[u, 0:64, :], ds_buf[...], ((1,), (0,)))
        dkv_ref[64:128, at] += dot(lt[u, 64:128, :], p_buf[...], ((1,), (0,)))

    for u in range(2):
        @pl.loop(0, diag[u])
        def _(t):
            main(u, t, False)

        main(u, diag[u], True)
        dq_ref[u] = (dq_acc[u] * SCORE_SCALE).astype(BF16)
    @pl.loop(0, key_tiles)
    def _(t):
        at = pl.ds(pl.multiple_of(t * TILE, TILE), TILE)
        dkv_ref[0:64, at] = dkv_ref[0:64, at] * SCORE_SCALE


def attention_grads(spans, qdo, delta, kv):
    rows = QUERY_PER_KEY * TILE
    keys = kv.shape[0]
    vmem = pl.BlockSpec(memory_space=pltpu.VMEM)
    return pl.pallas_call(
        functools.partial(compute_kernel, spans),
        out_shape=(
            jax.ShapeDtypeStruct((2, rows, LANES), BF16),
            jax.ShapeDtypeStruct((LANES, keys), F32),
        ),
        in_specs=[vmem] * 3,
        out_specs=(vmem, vmem),
        scratch_shapes=[
            pltpu.VMEM((2, 256, rows), BF16),
            pltpu.VMEM((2, QUERY_PER_KEY, TILE, LANES), BF16),
            pltpu.VMEM((keys, LANES), BF16),
            pltpu.VMEM((keys, LANES), BF16),
            pltpu.VMEM((keys, LANES), BF16),
            pltpu.VMEM((2, 8, rows), F32),
            pltpu.VMEM((2, 8, rows), F32),
            pltpu.VMEM((2, rows, LANES), F32),
            pltpu.VMEM((rows, TILE), BF16),
            pltpu.VMEM((rows, TILE), BF16),
        ],
        compiler_params=pltpu.CompilerParams(vmem_limit_bytes=60 * 1024 * 1024),
        name="attention_grads",
    )(qdo, delta, kv)


def per_device(queries, key_head_matrix, value_head_matrix, attn_output, out_grad):
    seqs = lax.axis_size("seq")
    spans = lax.axis_size("span")
    tokens = queries.shape[1]
    group = QUERY_PER_KEY * HEAD_WIDTH
    swap = [(i, spans - 1 - i) for i in range(spans)]

    q = queries.reshape(tokens, seqs, QUERY_PER_KEY, HEAD_WIDTH)
    do = out_grad.reshape(tokens, seqs, QUERY_PER_KEY, HEAD_WIDTH)
    o = attn_output.reshape(tokens, seqs, QUERY_PER_KEY, HEAD_WIDTH)
    qdo = jnp.transpose(jnp.concatenate([q, do], axis=3), (1, 2, 0, 3))
    delta = jnp.sum(do.astype(F32) * o.astype(F32), axis=3)
    delta = jnp.pad(jnp.transpose(delta, (1, 2, 0)), ((0, 0), (0, 5), (0, 0)))
    kv = jnp.concatenate(
        [
            key_head_matrix.reshape(tokens, seqs, HEAD_WIDTH),
            value_head_matrix.reshape(tokens, seqs, HEAD_WIDTH),
        ],
        axis=2,
    )
    kv = jnp.transpose(kv, (1, 0, 2))
    qdo = lax.all_to_all(qdo, "seq", split_axis=0, concat_axis=2, tiled=True)[0]
    delta = lax.all_to_all(delta, "seq", split_axis=0, concat_axis=2, tiled=True)[0]
    kv = lax.all_to_all(kv, "seq", split_axis=0, concat_axis=1, tiled=True)[0]
    kv = lax.all_gather(kv, "span", axis=0, tiled=True)
    qdo = jnp.stack([qdo[:, :TILE], lax.ppermute(qdo[:, TILE:], "span", swap)])
    delta = jnp.stack([delta[:, :TILE], lax.ppermute(delta[:, TILE:], "span", swap)])

    dq, dkv = attention_grads(spans, qdo, delta, kv)

    dkv = dkv.astype(BF16).reshape(LANES, spans, -1)
    dkv = lax.all_to_all(dkv, "span", split_axis=1, concat_axis=1, tiled=True)
    dkv = jnp.sum(dkv.astype(F32), axis=1).astype(BF16)
    dkv = jnp.transpose(dkv.reshape(LANES, seqs, tokens), (1, 2, 0))
    dkv = lax.all_to_all(dkv, "seq", split_axis=0, concat_axis=2, tiled=True)[0]
    dkv = dkv.reshape(tokens, seqs, 2, HEAD_WIDTH)
    dq = dq.reshape(2, QUERY_PER_KEY, TILE, LANES)[..., :HEAD_WIDTH]
    dq = jnp.transpose(dq, (0, 2, 1, 3)).reshape(2, TILE, group)
    dq = jnp.concatenate([dq[0], lax.ppermute(dq[1], "span", swap)], axis=0)
    dq = lax.all_to_all(dq.reshape(seqs, tokens, group), "seq", split_axis=0, concat_axis=2, tiled=True)
    return (
        dq,
        dkv[:, :, 0].reshape(1, tokens, seqs * HEAD_WIDTH),
        dkv[:, :, 1].reshape(1, tokens, seqs * HEAD_WIDTH),
    )


def solution(mesh):
    spec = P("span", "seq", None)
    return jax.shard_map(
        per_device, mesh=mesh, in_specs=(spec,) * 5, out_specs=(spec,) * 3, check_vma=False
    )
```

```python
import functools
import math

import jax
import jax.numpy as jnp
from jax import lax
from jax.experimental import pallas as pl
from jax.experimental.pallas import tpu as pltpu
from jax.sharding import PartitionSpec as P

HEAD_WIDTH = 64
QUERY_PER_KEY = 3
TILE = 512
CHUNK = 256
LANES = 128
NEG_LARGE = -1e30
SCORE_SCALE = 1.0 / math.sqrt(HEAD_WIDTH)
BASE2_SCALE = SCORE_SCALE * math.log2(math.e)
F32 = jnp.float32
BF16 = jnp.bfloat16


def dot(a, b, contract):
    return lax.dot_general(a, b, ((contract[0], contract[1]), ((), ())), preferred_element_type=F32)


def three_parts(x):
    first = x.astype(BF16).astype(F32)
    rest = x - first
    second = rest.astype(BF16).astype(F32)
    return first, second, rest - second


def fused_kernel(seqs, spans, q_in, k_in, v_in, o_in, do_in, qg_out, kg_out, vg_out, kv, qdo, delta, lt, l2, ks1, ks2, vs1, stat_m, stat_l,
                 dq_acc, p_buf, ds_buf, dkv_acc, kv_send, qdo_send, delta_send, part_send, part_recv, dq_send, dq_recv, grad_send, grad_recv,
                 kv_ss, kv_rs, qdo_ss, qdo_rs, delta_ss, delta_rs, cast_ss, cast_rs, part_ss, part_rs, dq_ss, dq_rs, grad_ss, grad_rs):
    own = lax.axis_index("span")
    seq = lax.axis_index("seq")
    tokens = q_in.shape[1]
    block_len = tokens * seqs
    half = seqs // 2
    rows = QUERY_PER_KEY * TILE
    key_tiles = kv.shape[0] // TILE
    mirror = spans - 1 - own
    unit = lax.div(seq, half)
    unit_span = jnp.where(unit == 0, own, mirror)
    unit_piece = lax.rem(seq, half)

    def needs(span, block):
        return block <= jnp.maximum(span, spans - 1 - span)

    def shifted(k, sign):
        z_step = lax.rem(k, 4)
        x_step = lax.rem(lax.div(k, 4) + z_step, 4)
        x = lax.rem(lax.div(own, 4) + 4 + sign * x_step, 4)
        z = lax.rem(lax.rem(own, 4) + 4 + sign * z_step, 4)
        return x * 4 + z

    def seq_shifted(k, sign):
        return lax.rem(seq + seqs + sign * k, seqs)

    def remote(source, target, send, receive, span, at_seq):
        return pltpu.make_async_remote_copy(
            src_ref=source, dst_ref=target, send_sem=send, recv_sem=receive,
            device_id={"span": span, "seq": at_seq}, device_id_type=pl.DeviceIdType.MESH,
        )

    barrier = pltpu.get_barrier_semaphore()

    def greet(span, at_seq):
        pl.semaphore_signal(barrier, inc=1, device_id={"span": span, "seq": at_seq}, device_id_type=pl.DeviceIdType.MESH)

    for k in range(1, seqs):
        greet(own, seq_shifted(k, 1))
    for k in range(seqs):
        greet(mirror, seq_shifted(k, 1))

    @pl.loop(1, spans)
    def _(k):
        there = shifted(k, 1)

        @pl.when(there != mirror)
        def _():
            greet(there, seq)

    lane = lax.broadcasted_iota(jnp.int32, (tokens, LANES), 1)
    low = lane < HEAD_WIDTH

    def columns(ref, i):
        return ref[0, :, i * LANES : (i + 1) * LANES].astype(F32)

    def paired(a, b):
        return (
            jnp.where(low, a, pltpu.roll(b, HEAD_WIDTH, 1)).astype(BF16),
            jnp.where(low, pltpu.roll(a, HEAD_WIDTH, 1), b).astype(BF16),
        )

    for i in range(seqs // 2):
        kv_send[2 * i], kv_send[2 * i + 1] = paired(columns(k_in, i), columns(v_in, i))

    pl.semaphore_wait(barrier, (seqs - 1) + seqs + (spans - 2))

    def kv_copy(k):
        there = seq_shifted(k, 1)
        at = pl.ds(pl.multiple_of(own * block_len + seq * tokens, tokens), tokens)
        return remote(kv_send.at[there], kv.at[at], kv_ss.at[k], kv_rs.at[k], own, there)

    for k in range(1, seqs):
        kv_copy(k).start()
    kv[pl.ds(pl.multiple_of(own * block_len + seq * tokens, tokens), tokens), :] = kv_send[seq]

    heads = seqs * QUERY_PER_KEY
    for i in range(heads // 2):
        a, b = paired(columns(q_in, i), columns(do_in, i))
        n = 2 * i
        qdo_send[n // QUERY_PER_KEY, n % QUERY_PER_KEY] = a
        n = 2 * i + 1
        qdo_send[n // QUERY_PER_KEY, n % QUERY_PER_KEY] = b

    def qdo_copy(k):
        there = seq_shifted(k, 1)
        at = pl.ds(pl.multiple_of(unit_piece * tokens, tokens), tokens)
        return remote(qdo_send.at[there], qdo.at[unit, :, at, :], qdo_ss.at[k], qdo_rs.at[k], unit_span, there)

    def delta_copy(k):
        there = seq_shifted(k, 1)
        return remote(
            delta_send.at[pl.ds(pl.multiple_of(there * 8, 8), 8), :], delta.at[unit, unit_piece],
            delta_ss.at[k], delta_rs.at[k], unit_span, there,
        )

    for k in range(1, seqs):
        qdo_copy(k).start()

    @pl.when(unit == 0)
    def _():
        qdo[0, :, pl.ds(pl.multiple_of(unit_piece * tokens, tokens), tokens), :] = qdo_send[seq]

    @pl.when(unit != 0)
    def _():
        qdo_copy(0).start()

    for k in range(1, seqs):
        kv_copy(k).wait_recv()

    def cast_copy(k):
        at = pl.ds(pl.multiple_of(own * block_len, block_len), block_len)
        return remote(kv.at[at], kv.at[at], cast_ss.at[k], cast_rs.at[k], shifted(k, 1), seq)

    def cast_wait(k):
        at = pl.ds(pl.multiple_of(shifted(k, -1) * block_len, block_len), block_len)
        remote(kv.at[at], kv.at[at], cast_ss.at[k], cast_rs.at[k], shifted(k, 1), seq).wait_recv()

    @pl.loop(1, spans)
    def _(k):
        @pl.when(needs(shifted(k, 1), own))
        def _():
            cast_copy(k).start()

    head_row = lax.broadcasted_iota(jnp.int32, (8 * seqs, heads * HEAD_WIDTH), 0)
    head_col = lax.broadcasted_iota(jnp.int32, (8 * seqs, heads * HEAD_WIDTH), 1)
    in_group = head_row - lax.shift_left(lax.shift_right_logical(head_row, 3), 3)
    wanted = lax.shift_right_logical(head_row, 3) * QUERY_PER_KEY + in_group
    member = (in_group < QUERY_PER_KEY) & (wanted == lax.shift_right_logical(head_col, 6))
    selector = jnp.where(member, 1.0, 0.0).astype(BF16)
    product = do_in[0].astype(F32) * o_in[0].astype(F32)
    product_high = product.astype(BF16)
    product_low = (product - product_high.astype(F32)).astype(BF16)
    delta_send[...] = dot(selector, product_high, ((1,), (1,))) + dot(selector, product_low, ((1,), (1,)))
    for k in range(1, seqs):
        delta_copy(k).start()

    @pl.when(unit == 0)
    def _():
        delta[0, unit_piece] = delta_send[pl.ds(pl.multiple_of(seq * 8, 8), 8), :]

    @pl.when(unit != 0)
    def _():
        delta_copy(0).start()

    def from_everyone(copies):
        for k in range(1, seqs):
            copies(k).wait_recv()

        @pl.when(unit != 0)
        def _():
            copies(0).wait_recv()

    from_everyone(qdo_copy)

    @pl.loop(0, 2)
    def _(u):
        for h in range(QUERY_PER_KEY):
            cols = pl.ds(h * TILE, TILE)
            turned = qdo[u, h].astype(F32).T
            lt[u, 0:128, cols] = turned.astype(BF16)
            lt[u, 128:256, cols] = jnp.concatenate([turned[0:64], jnp.zeros((64, TILE), F32)], axis=0).astype(BF16)
        dq_acc[u] = jnp.zeros((rows, LANES), F32)
        stat_m[u] = jnp.full((8, rows), NEG_LARGE, F32)
        stat_l[u] = jnp.zeros((8, rows), F32)

    key_lane = lax.broadcasted_iota(jnp.int32, (TILE, LANES), 1)
    aux_s = jnp.where((key_lane >= 64) & (key_lane < 67), -1.0, 0.0)
    aux_v = jnp.where((key_lane >= 67) & (key_lane < 70), -1.0, 0.0).astype(BF16)

    def prepare(t):
        at = pl.ds(pl.multiple_of(t * TILE, TILE), TILE)
        raw = kv[at, :].astype(F32)
        scaled = raw * BASE2_SCALE
        high = scaled.astype(BF16).astype(F32)
        ks1[at, :] = jnp.where(key_lane < 64, high, 0.0).astype(BF16)
        ks2[at, :] = jnp.where(key_lane < 64, scaled - high, aux_s).astype(BF16)
        vs1[at, :] = jnp.where(key_lane >= 64, raw, 0.0).astype(BF16)

    def stats(u, t, masked):
        at = pl.ds(pl.multiple_of(t * TILE, TILE), TILE)
        w = jnp.concatenate([ks1[at, :], ks2[at, :]], axis=1)
        for h in range(QUERY_PER_KEY):
            cols = pl.ds(h * TILE, TILE)
            s = dot(w, lt[u, :, cols], ((1,), (0,)))
            if masked:
                key_at = lax.broadcasted_iota(jnp.int32, (TILE, TILE), 0)
                query_at = lax.broadcasted_iota(jnp.int32, (TILE, TILE), 1)
                s = jnp.where(key_at <= query_at, s, NEG_LARGE)
            old = stat_m[u, 0:1, cols]
            new = jnp.maximum(old, jnp.max(s, axis=0, keepdims=True))
            e = jnp.exp2(s - new)
            part = jnp.sum(e.reshape(TILE // 8, 8, TILE), axis=0)
            stat_l[u, :, cols] = stat_l[u, :, cols] * jnp.exp2(old - new) + part
            stat_m[u, :, cols] = jnp.broadcast_to(new, (8, TILE))

    def visit(block, step):
        @pl.loop(0, 4)
        def _(i):
            u = lax.rem(i, 2)
            t = block * 2 + lax.div(i, 2)
            last = jnp.where(u == 0, 2 * own, key_tiles - 1 - 2 * own)

            @pl.when(t < last)
            def _():
                step(u, t, False)

            @pl.when(t == last)
            def _():
                step(u, t, True)

    @pl.loop(0, spans)
    def _(k):
        block = shifted(k, -1)

        @pl.when(needs(own, block))
        def _():
            @pl.when(k > 0)
            def _():
                cast_wait(k)

            prepare(2 * block)
            prepare(2 * block + 1)
            visit(block, stats)

    from_everyone(delta_copy)
    row = lax.broadcasted_iota(jnp.int32, (16, TILE), 0)

    @pl.loop(0, 2)
    def _(u):
        for h in range(QUERY_PER_KEY):
            cols = pl.ds(h * TILE, TILE)
            total = jnp.sum(stat_l[u, :, cols], axis=0, keepdims=True)
            lse = stat_m[u, 0:1, cols] + jnp.log2(total)
            shifts = jnp.concatenate([delta[u, i, h : h + 1, :] for i in range(half)], axis=1)
            parts = three_parts(lse) + three_parts(shifts)
            block = jnp.zeros((16, TILE), F32)
            for i, part in enumerate(parts):
                block = jnp.where(row == i, part, block)
            lt[u, 192:208, cols] = block.astype(BF16)
            l2[u, h] = lt[u, 128:256, cols].astype(F32).T.astype(BF16)

    def main(u, t, masked):
        at = pl.ds(pl.multiple_of(t * TILE, TILE), TILE)
        within = pl.ds(pl.multiple_of(lax.rem(t, 2) * TILE, TILE), TILE)
        kw = jnp.concatenate([ks1[at, :], ks2[at, :]], axis=1)
        vw = jnp.concatenate([vs1[at, :], aux_v], axis=1)
        raw = kv[at, :]
        if masked:
            key_col = lax.broadcasted_iota(jnp.int32, (CHUNK, TILE), 1)
            query_row = lax.broadcasted_iota(jnp.int32, (CHUNK, TILE), 0)
        for h in range(QUERY_PER_KEY):
            for first in range(0, TILE, CHUNK):
                here = pl.ds(h * TILE + first, CHUNK)
                lhs = jnp.concatenate([qdo[u, h, first : first + CHUNK, :], l2[u, h, first : first + CHUNK, :]], axis=1)
                s = dot(lhs, kw, ((1,), (1,)))
                dp = dot(lhs, vw, ((1,), (1,)))
                p = jnp.exp2(s)
                if masked:
                    p = jnp.where(key_col <= query_row + first, p, 0.0)
                ds = (p * dp).astype(BF16)
                p_buf[here, :] = p.astype(BF16)
                ds_buf[here, :] = ds
                dq_acc[u, here, :] += dot(ds, raw, ((1,), (0,)))
        dkv_acc[0:64, within] += dot(lt[u, 0:64, :], ds_buf[...], ((1,), (0,)))
        dkv_acc[64:128, within] += dot(lt[u, 64:128, :], p_buf[...], ((1,), (0,)))

    def part_copy(k):
        return remote(part_send.at[k], part_recv.at[k], part_ss.at[k], part_rs.at[k], shifted(k, -1), seq)

    @pl.loop(1, spans + 1)
    def _(j):
        k = lax.rem(j, spans)
        block = shifted(k, -1)

        @pl.when(needs(own, block))
        def _():
            dkv_acc[...] = jnp.zeros((LANES, block_len), F32)
            visit(block, main)
            dkv_acc[0:64, :] = dkv_acc[0:64, :] * SCORE_SCALE

            @pl.when(k > 0)
            def _():
                part_send[k] = dkv_acc[...].astype(BF16)
                part_copy(k).start()

    even = lax.rem(seq, 2) == 0

    def dq_copy(j):
        u, i = j // half, j % half
        at_span = own if u == 0 else mirror
        return remote(dq_send.at[j], dq_recv.at[seq], dq_ss.at[j], dq_rs.at[seq], at_span, j)

    def dq_arrival(g):
        return remote(dq_send.at[0], dq_recv.at[g], dq_ss.at[0], dq_rs.at[g], own, g)

    for j in range(seqs):
        u, i = j // half, j % half
        h0, h1, h2 = (dq_acc[u, h * TILE + i * tokens : h * TILE + (i + 1) * tokens, :] * SCORE_SCALE for h in range(QUERY_PER_KEY))
        middle = pltpu.roll(h1, HEAD_WIDTH, 1)
        first = jnp.where(even, jnp.where(low, h0, middle), pltpu.roll(h0, HEAD_WIDTH, 1))
        second = jnp.where(even, h2, jnp.where(low, h1, pltpu.roll(h2, HEAD_WIDTH, 1)))
        dq_send[j, 0] = first.astype(BF16)
        dq_send[j, 1] = second.astype(BF16)
        if u == 0:
            @pl.when(seq == j)
            def _():
                dq_recv[j] = dq_send[j]

            @pl.when(seq != j)
            def _():
                dq_copy(j).start()
        else:
            dq_copy(j).start()

    @pl.loop(1, spans)
    def _(k):
        @pl.when(needs(shifted(k, 1), own))
        def _():
            part_copy(k).wait_recv()
            dkv_acc[...] += part_recv[k].astype(F32)

    def grad_copy(k):
        there = seq_shifted(k, 1)
        return remote(grad_send.at[k], grad_recv.at[k], grad_ss.at[k], grad_rs.at[k], own, there)

    for k in range(seqs):
        there = seq_shifted(k, 1)
        piece = dkv_acc[:, pl.ds(pl.multiple_of(there * tokens, tokens), tokens)].T.astype(BF16)
        if k == 0:
            grad_recv[0] = piece
        else:
            grad_send[k] = piece
            grad_copy(k).start()

    for g in range(seqs):
        remote_here = jnp.logical_or(unit != 0, seq != g)

        @pl.when(remote_here)
        def _():
            dq_arrival(g).wait_recv()

    for i in range(seqs // 2):
        at = 3 * LANES * i
        qg_out[0, :, at : at + LANES] = dq_recv[2 * i, 0]
        both = jnp.where(low, dq_recv[2 * i, 1].astype(F32), dq_recv[2 * i + 1, 0].astype(F32))
        qg_out[0, :, at + LANES : at + 2 * LANES] = both.astype(BF16)
        qg_out[0, :, at + 2 * LANES : at + 3 * LANES] = dq_recv[2 * i + 1, 1]

    for k in range(1, seqs):
        grad_copy(k).wait_recv()
    for i in range(seqs // 2):
        a = grad_recv[lax.rem(seq + seqs - 2 * i, seqs)]
        b = grad_recv[lax.rem(seq + seqs - 2 * i - 1, seqs)]
        key_part, value_part = paired(a.astype(F32), b.astype(F32))
        kg_out[0, :, i * LANES : (i + 1) * LANES] = key_part
        vg_out[0, :, i * LANES : (i + 1) * LANES] = value_part

    for k in range(1, seqs):
        kv_copy(k).wait_send()
        qdo_copy(k).wait_send()
        delta_copy(k).wait_send()
        grad_copy(k).wait_send()

    @pl.when(unit != 0)
    def _():
        qdo_copy(0).wait_send()
        delta_copy(0).wait_send()

    for j in range(seqs):
        if j < half:
            @pl.when(seq != j)
            def _():
                dq_copy(j).wait_send()
        else:
            dq_copy(j).wait_send()

    @pl.loop(1, spans)
    def _(k):
        @pl.when(needs(shifted(k, 1), own))
        def _():
            cast_copy(k).wait_send()

        @pl.when(needs(own, shifted(k, -1)))
        def _():
            part_copy(k).wait_send()


def solution(mesh):
    seqs, spans = mesh.shape["seq"], mesh.shape["span"]
    spec = P("span", "seq", None)

    def per_device(queries, keys, values, attn_output, out_grad):
        tokens = queries.shape[1]
        block_len = tokens * seqs
        total = block_len * spans
        rows = QUERY_PER_KEY * TILE
        vmem = pl.BlockSpec(memory_space=pltpu.VMEM)
        dma = pltpu.SemaphoreType.DMA
        return pl.pallas_call(
            functools.partial(fused_kernel, seqs, spans),
            out_shape=(
                jax.ShapeDtypeStruct(queries.shape, BF16),
                jax.ShapeDtypeStruct(keys.shape, BF16),
                jax.ShapeDtypeStruct(values.shape, BF16),
            ),
            in_specs=[vmem] * 5,
            out_specs=(vmem,) * 3,
            scratch_shapes=[
                pltpu.VMEM((total, LANES), BF16),
                pltpu.VMEM((2, QUERY_PER_KEY, TILE, LANES), BF16),
                pltpu.VMEM((2, seqs // 2, 8, tokens), F32),
                pltpu.VMEM((2, 256, rows), BF16),
                pltpu.VMEM((2, QUERY_PER_KEY, TILE, LANES), BF16),
                pltpu.VMEM((total, LANES), BF16),
                pltpu.VMEM((total, LANES), BF16),
                pltpu.VMEM((total, LANES), BF16),
                pltpu.VMEM((2, 8, rows), F32),
                pltpu.VMEM((2, 8, rows), F32),
                pltpu.VMEM((2, rows, LANES), F32),
                pltpu.VMEM((rows, TILE), BF16),
                pltpu.VMEM((rows, TILE), BF16),
                pltpu.VMEM((LANES, block_len), F32),
                pltpu.VMEM((seqs, tokens, LANES), BF16),
                pltpu.VMEM((seqs, QUERY_PER_KEY, tokens, LANES), BF16),
                pltpu.VMEM((8 * seqs, tokens), F32),
                pltpu.VMEM((spans, LANES, block_len), BF16),
                pltpu.VMEM((spans, LANES, block_len), BF16),
                pltpu.VMEM((seqs, 2, tokens, LANES), BF16),
                pltpu.VMEM((seqs, 2, tokens, LANES), BF16),
                pltpu.VMEM((seqs, tokens, LANES), BF16),
                pltpu.VMEM((seqs, tokens, LANES), BF16),
            ]
            + [dma((seqs,))] * 6 + [dma((spans,))] * 4 + [dma((seqs,))] * 4,
            compiler_params=pltpu.CompilerParams(
                vmem_limit_bytes=60 * 1024 * 1024, collective_id=0, has_side_effects=True
            ),
            name="attention_grads",
        )(queries, keys, values, attn_output, out_grad)

    return jax.shard_map(
        per_device, mesh=mesh, in_specs=(spec,) * 5, out_specs=(spec,) * 3, check_vma=False
    )
```

```python
import functools
import math

import jax
import jax.numpy as jnp
from jax import lax
from jax.experimental import pallas as pl
from jax.experimental.pallas import tpu as pltpu
from jax.sharding import PartitionSpec as P

HEAD_WIDTH = 64
QUERY_PER_KEY = 3
TILE = 512
HALF = TILE // 2
LANES = 128
NEG_LARGE = -1e30
SCORE_SCALE = 1.0 / math.sqrt(HEAD_WIDTH)
BASE2_SCALE = SCORE_SCALE * math.log2(math.e)
F32 = jnp.float32
BF16 = jnp.bfloat16


def dot(a, b, contract):
    return lax.dot_general(a, b, ((contract[0], contract[1]), ((), ())), preferred_element_type=F32)


def three_parts(x):
    first = x.astype(BF16).astype(F32)
    rest = x - first
    second = rest.astype(BF16).astype(F32)
    return first, second, rest - second


def fused_kernel(seqs, spans, q_in, k_in, v_in, o_in, do_in, qg_out, kg_out, vg_out, k_got, v_got, q_got, do_got, delta, lt, l1, l2, k_rows,
                 ks_t, vs_t, ks, stat_m, stat_l, dq_acc, p_buf, ds_buf, dkv_acc, k_send, v_send, q_send, do_send, delta_send,
                 part_send, part_recv, dq_send, dq_recv, grad_send, grad_recv, k_ss, k_rs, v_ss, v_rs, q_ss, q_rs, do_ss, do_rs,
                 delta_ss, delta_rs, kcast_ss, kcast_rs, vcast_ss, vcast_rs, part_ss, part_rs, dq_ss, dq_rs, grad_ss, grad_rs):
    own = lax.axis_index("span")
    seq = lax.axis_index("seq")
    tokens = q_in.shape[1]
    block_len = tokens * seqs
    half = seqs // 2
    rows = QUERY_PER_KEY * TILE
    key_tiles = k_rows.shape[0] // TILE
    packed = tokens // 2
    mirror = spans - 1 - own
    unit = lax.div(seq, half)
    unit_span = jnp.where(unit == 0, own, mirror)
    unit_piece = lax.rem(seq, half)

    def needs(span, block):
        return block <= jnp.maximum(span, spans - 1 - span)

    def shifted(k, sign):
        z_step = lax.rem(k, 4)
        x_step = lax.rem(lax.div(k, 4) + z_step, 4)
        x = lax.rem(lax.div(own, 4) + 4 + sign * x_step, 4)
        z = lax.rem(lax.rem(own, 4) + 4 + sign * z_step, 4)
        return x * 4 + z

    def seq_shifted(k, sign):
        return lax.rem(seq + seqs + sign * k, seqs)

    def remote(source, target, send, receive, span, at_seq):
        return pltpu.make_async_remote_copy(
            src_ref=source, dst_ref=target, send_sem=send, recv_sem=receive,
            device_id={"span": span, "seq": at_seq}, device_id_type=pl.DeviceIdType.MESH,
        )

    barrier = pltpu.get_barrier_semaphore()

    def greet(span, at_seq):
        pl.semaphore_signal(barrier, inc=1, device_id={"span": span, "seq": at_seq}, device_id_type=pl.DeviceIdType.MESH)

    for k in range(1, seqs):
        greet(own, seq_shifted(k, 1))
    for k in range(seqs):
        greet(mirror, seq_shifted(k, 1))

    @pl.loop(1, spans)
    def _(k):
        there = shifted(k, 1)

        @pl.when(there != mirror)
        def _():
            greet(there, seq)

    lane = lax.broadcasted_iota(jnp.int32, (tokens, LANES), 1)
    low = lane < HEAD_WIDTH

    def paired(a, b):
        mask = lax.broadcasted_iota(jnp.int32, a.shape, 1) < HEAD_WIDTH
        return (
            jnp.where(mask, a, pltpu.roll(b, HEAD_WIDTH, 1)).astype(BF16),
            jnp.where(mask, pltpu.roll(a, HEAD_WIDTH, 1), b).astype(BF16),
        )

    def pack(ref, i):
        at = slice(i * LANES, (i + 1) * LANES)
        return paired(ref[0, :packed, at].astype(F32), ref[0, packed:, at].astype(F32))

    heads = seqs * QUERY_PER_KEY

    def pack_keys(ref, out):
        for i in range(seqs // 2):
            out[2 * i], out[2 * i + 1] = pack(ref, i)

    def pack_queries(ref, out):
        for i in range(heads // 2):
            a, b = pack(ref, i)
            n = 2 * i
            out[n // QUERY_PER_KEY, n % QUERY_PER_KEY] = a
            n = 2 * i + 1
            out[n // QUERY_PER_KEY, n % QUERY_PER_KEY] = b

    pack_keys(k_in, k_send)
    pl.semaphore_wait(barrier, (seqs - 1) + seqs + (spans - 2))

    own_rows = pl.ds(pl.multiple_of(own * (block_len // 2) + seq * packed, packed), packed)
    unit_rows = pl.ds(pl.multiple_of(unit_piece * packed, packed), packed)

    def k_copy(k):
        there = seq_shifted(k, 1)
        return remote(k_send.at[there], k_got.at[own_rows], k_ss.at[k], k_rs.at[k], own, there)

    def v_copy(k):
        there = seq_shifted(k, 1)
        return remote(v_send.at[there], v_got.at[own_rows], v_ss.at[k], v_rs.at[k], own, there)

    def q_copy(k):
        there = seq_shifted(k, 1)
        return remote(q_send.at[there], q_got.at[unit, :, unit_rows, :], q_ss.at[k], q_rs.at[k], unit_span, there)

    def do_copy(k):
        there = seq_shifted(k, 1)
        return remote(do_send.at[there], do_got.at[unit, :, unit_rows, :], do_ss.at[k], do_rs.at[k], unit_span, there)

    def delta_copy(k):
        there = seq_shifted(k, 1)
        return remote(
            delta_send.at[pl.ds(pl.multiple_of(there * 8, 8), 8), :], delta.at[unit, unit_piece],
            delta_ss.at[k], delta_rs.at[k], unit_span, there,
        )

    def cast_copy(k, got, send, receive):
        at = pl.ds(pl.multiple_of(own * (block_len // 2), block_len // 2), block_len // 2)
        return remote(got.at[at], got.at[at], send.at[k], receive.at[k], shifted(k, 1), seq)

    def k_cast(k):
        return cast_copy(k, k_got, kcast_ss, kcast_rs)

    def v_cast(k):
        return cast_copy(k, v_got, vcast_ss, vcast_rs)

    def cast_all(cast):
        @pl.loop(1, spans)
        def _(k):
            @pl.when(needs(shifted(k, 1), own))
            def _():
                cast(k).start()

    for k in range(1, seqs):
        k_copy(k).start()
    k_got[own_rows, :] = k_send[seq]
    pack_queries(q_in, q_send)
    for k in range(1, seqs):
        q_copy(k).start()

    @pl.when(unit == 0)
    def _():
        q_got[0, :, unit_rows, :] = q_send[seq]

    @pl.when(unit != 0)
    def _():
        q_copy(0).start()

    for k in range(1, seqs):
        k_copy(k).wait_recv()
    cast_all(k_cast)

    pack_keys(v_in, v_send)
    for k in range(1, seqs):
        v_copy(k).start()
    v_got[own_rows, :] = v_send[seq]
    pack_queries(do_in, do_send)
    for k in range(1, seqs):
        do_copy(k).start()

    @pl.when(unit == 0)
    def _():
        do_got[0, :, unit_rows, :] = do_send[seq]

    @pl.when(unit != 0)
    def _():
        do_copy(0).start()

    head_row = lax.broadcasted_iota(jnp.int32, (8 * seqs, heads * HEAD_WIDTH), 0)
    head_col = lax.broadcasted_iota(jnp.int32, (8 * seqs, heads * HEAD_WIDTH), 1)
    in_group = head_row - lax.shift_left(lax.shift_right_logical(head_row, 3), 3)
    wanted = lax.shift_right_logical(head_row, 3) * QUERY_PER_KEY + in_group
    member = (in_group < QUERY_PER_KEY) & (wanted == lax.shift_right_logical(head_col, 6))
    selector = jnp.where(member, 1.0, 0.0).astype(BF16)
    product = do_in[0].astype(F32) * o_in[0].astype(F32)
    product_high = product.astype(BF16)
    product_low = (product - product_high.astype(F32)).astype(BF16)
    delta_send[...] = dot(selector, product_high, ((1,), (1,))) + dot(selector, product_low, ((1,), (1,)))
    for k in range(1, seqs):
        delta_copy(k).start()

    @pl.when(unit == 0)
    def _():
        delta[0, unit_piece] = delta_send[pl.ds(pl.multiple_of(seq * 8, 8), 8), :]

    @pl.when(unit != 0)
    def _():
        delta_copy(0).start()

    def from_everyone(copies):
        for k in range(1, seqs):
            copies(k).wait_recv()

        @pl.when(unit != 0)
        def _():
            copies(0).wait_recv()

    from_everyone(q_copy)

    def halves(x):
        return jnp.concatenate([x[0:HEAD_WIDTH], x[HEAD_WIDTH:]], axis=1)

    @pl.loop(0, 2)
    def _(u):
        for h in range(QUERY_PER_KEY):
            cols = pl.ds(h * TILE, TILE)
            turned = halves(q_got[u, h].astype(F32).T).astype(BF16)
            nothing = jnp.zeros((HEAD_WIDTH, TILE), BF16)
            lt[u, 0:64, cols] = turned
            lt[u, 64:128, cols] = nothing
            lt[u, 128:192, cols] = turned
            lt[u, 192:256, cols] = nothing
        dq_acc[u] = jnp.zeros((rows, LANES), F32)
        stat_m[u] = jnp.full((8, rows), NEG_LARGE, F32)
        stat_l[u] = jnp.zeros((8, rows), F32)

    aux_row = lax.broadcasted_iota(jnp.int32, (HEAD_WIDTH, TILE), 0)
    aux_s = jnp.where(aux_row < 3, -1.0, 0.0)
    aux_v = jnp.where((aux_row >= 3) & (aux_row < 6), -1.0, 0.0)

    def packed_tile(got, t):
        return got[pl.ds(pl.multiple_of(t * HALF, HALF), HALF), :].astype(F32)

    def prepare_keys(t):
        at = pl.ds(pl.multiple_of(t * TILE, TILE), TILE)
        raw = packed_tile(k_got, t)
        zero = jnp.zeros((HALF, LANES), F32)
        mask = lax.broadcasted_iota(jnp.int32, (HALF, LANES), 1) < HEAD_WIDTH

        def spread(x):
            return jnp.concatenate([jnp.where(mask, x, zero), jnp.where(mask, pltpu.roll(x, HEAD_WIDTH, 1), zero)], axis=0)

        k_rows[at, :] = spread(raw).astype(BF16)
        scaled = raw * BASE2_SCALE
        high = scaled.astype(BF16).astype(F32)
        rest = scaled - high
        within = pl.ds(pl.multiple_of(lax.rem(t, 2) * TILE, TILE), TILE)
        ks[within, 0:128] = spread(high).astype(BF16)
        ks[within, 128:256] = spread(rest).astype(BF16)
        nothing = jnp.zeros((HEAD_WIDTH, TILE), F32)
        ks_t[0:128, at] = jnp.concatenate([halves(high.T), nothing], axis=0).astype(BF16)
        ks_t[128:256, at] = jnp.concatenate([halves(rest.T), aux_s], axis=0).astype(BF16)

    def prepare_values(t):
        at = pl.ds(pl.multiple_of(t * TILE, TILE), TILE)
        nothing = jnp.zeros((HEAD_WIDTH, TILE), F32)
        vs_t[0:128, at] = jnp.concatenate([nothing, halves(packed_tile(v_got, t).T)], axis=0).astype(BF16)
        vs_t[128:256, at] = jnp.concatenate([nothing, aux_v], axis=0).astype(BF16)

    def place(axis):
        r = lax.broadcasted_iota(jnp.int32, (TILE, TILE), axis)
        quarter = lax.shift_right_logical(r & (HALF - 1), 6)
        return quarter * 128 + lax.shift_right_logical(r, 8) * 64 + (r & 63)

    def stats(u, t, masked):
        w = ks[pl.ds(pl.multiple_of(lax.rem(t, 2) * TILE, TILE), TILE), :]
        for h in range(QUERY_PER_KEY):
            cols = pl.ds(h * TILE, TILE)
            s = dot(w, lt[u, :, cols], ((1,), (0,)))
            if masked:
                s = jnp.where(place(0) <= place(1), s, NEG_LARGE)
            old = stat_m[u, 0:1, cols]
            new = jnp.maximum(old, jnp.max(s, axis=0, keepdims=True))
            e = jnp.exp2(s - new)
            part = jnp.sum(e.reshape(TILE // 8, 8, TILE), axis=0)
            stat_l[u, :, cols] = stat_l[u, :, cols] * jnp.exp2(old - new) + part
            stat_m[u, :, cols] = jnp.broadcast_to(new, (8, TILE))

    def visit(block, step):
        @pl.loop(0, 4)
        def _(i):
            u = lax.rem(i, 2)
            t = block * 2 + lax.div(i, 2)
            last = jnp.where(u == 0, 2 * own, key_tiles - 1 - 2 * own)

            @pl.when(t < last)
            def _():
                step(u, t, False)

            @pl.when(t == last)
            def _():
                step(u, t, True)

    def cast_wait(k, got, send, receive):
        at = pl.ds(pl.multiple_of(shifted(k, -1) * (block_len // 2), block_len // 2), block_len // 2)
        remote(got.at[at], got.at[at], send.at[k], receive.at[k], shifted(k, 1), seq).wait_recv()

    @pl.loop(0, spans)
    def _(k):
        block = shifted(k, -1)

        @pl.when(needs(own, block))
        def _():
            @pl.when(k > 0)
            def _():
                cast_wait(k, k_got, kcast_ss, kcast_rs)

            prepare_keys(2 * block)
            prepare_keys(2 * block + 1)
            visit(block, stats)

            @pl.when(k == 0)
            def _():
                for i in range(1, seqs):
                    v_copy(i).wait_recv()
                cast_all(v_cast)

    from_everyone(delta_copy)
    from_everyone(do_copy)
    row = lax.broadcasted_iota(jnp.int32, (16, TILE), 0)

    @pl.loop(0, 2)
    def _(u):
        for h in range(QUERY_PER_KEY):
            cols = pl.ds(h * TILE, TILE)
            total = jnp.sum(stat_l[u, :, cols], axis=0, keepdims=True)
            lse = stat_m[u, 0:1, cols] + jnp.log2(total)
            pieces = [delta[u, i, h : h + 1, :] for i in range(half)]
            shifts = jnp.concatenate([x[:, :packed] for x in pieces] + [x[:, packed:] for x in pieces], axis=1)
            parts = three_parts(lse) + three_parts(shifts)
            block = jnp.zeros((16, TILE), F32)
            for i, part in enumerate(parts):
                block = jnp.where(row == i, part, block)
            lt[u, 192:208, cols] = block.astype(BF16)
            lt[u, 64:128, cols] = halves(do_got[u, h].astype(F32).T).astype(BF16)
            l1[u, h, :HALF, :], l1[u, h, HALF:, :] = paired(q_got[u, h].astype(F32), do_got[u, h].astype(F32))
            l2[u, h] = lt[u, 128:256, cols].astype(F32).T.astype(BF16)

    def main(u, t, masked):
        at = pl.ds(pl.multiple_of(t * TILE, TILE), TILE)
        within = pl.ds(pl.multiple_of(lax.rem(t, 2) * TILE, TILE), TILE)
        kw = ks_t[:, at]
        vw = vs_t[:, at]
        raw = k_rows[at, :]
        for h in range(QUERY_PER_KEY):
            here = pl.ds(h * TILE, TILE)
            lhs = jnp.concatenate([l1[u, h], l2[u, h]], axis=1)
            s = dot(lhs, kw, ((1,), (0,)))
            dp = dot(lhs, vw, ((1,), (0,)))
            p = jnp.exp2(s)
            if masked:
                p = jnp.where(place(1) <= place(0), p, 0.0)
            ds = (p * dp).astype(BF16)
            p_buf[here, :] = p.astype(BF16)
            ds_buf[here, :] = ds
            dq_acc[u, here, :] += dot(ds, raw, ((1,), (0,)))
        dkv_acc[0:64, within] += dot(lt[u, 0:64, :], ds_buf[...], ((1,), (0,)))
        dkv_acc[64:128, within] += dot(lt[u, 64:128, :], p_buf[...], ((1,), (0,)))

    def part_copy(k):
        return remote(part_send.at[k], part_recv.at[k], part_ss.at[k], part_rs.at[k], shifted(k, -1), seq)

    @pl.loop(1, spans + 1)
    def _(j):
        k = lax.rem(j, spans)
        block = shifted(k, -1)

        @pl.when(needs(own, block))
        def _():
            @pl.when(k > 0)
            def _():
                cast_wait(k, v_got, vcast_ss, vcast_rs)

            prepare_values(2 * block)
            prepare_values(2 * block + 1)
            dkv_acc[...] = jnp.zeros((LANES, block_len), F32)
            visit(block, main)
            dkv_acc[0:64, :] = dkv_acc[0:64, :] * SCORE_SCALE

            @pl.when(k > 0)
            def _():
                part_send[k] = dkv_acc[...].astype(BF16)
                part_copy(k).start()

    even = lax.rem(seq, 2) == 0

    def dq_copy(j):
        u, i = j // half, j % half
        at_span = own if u == 0 else mirror
        return remote(dq_send.at[j], dq_recv.at[seq], dq_ss.at[j], dq_rs.at[seq], at_span, j)

    def dq_arrival(g):
        return remote(dq_send.at[0], dq_recv.at[g], dq_ss.at[0], dq_rs.at[g], own, g)

    for j in range(seqs):
        u, i = j // half, j % half
        h0, h1, h2 = (
            jnp.concatenate([dq_acc[u, at : at + packed, :], dq_acc[u, at + HALF : at + HALF + packed, :]], axis=0) * SCORE_SCALE
            for at in (h * TILE + i * packed for h in range(QUERY_PER_KEY))
        )
        middle = pltpu.roll(h1, HEAD_WIDTH, 1)
        first = jnp.where(even, jnp.where(low, h0, middle), pltpu.roll(h0, HEAD_WIDTH, 1))
        second = jnp.where(even, h2, jnp.where(low, h1, pltpu.roll(h2, HEAD_WIDTH, 1)))
        dq_send[j, 0] = first.astype(BF16)
        dq_send[j, 1] = second.astype(BF16)
        if u == 0:
            @pl.when(seq == j)
            def _():
                dq_recv[j] = dq_send[j]

            @pl.when(seq != j)
            def _():
                dq_copy(j).start()
        else:
            dq_copy(j).start()

    @pl.loop(1, spans)
    def _(k):
        @pl.when(needs(shifted(k, 1), own))
        def _():
            part_copy(k).wait_recv()
            dkv_acc[...] += part_recv[k].astype(F32)

    def grad_copy(k):
        there = seq_shifted(k, 1)
        return remote(grad_send.at[there], grad_recv.at[k], grad_ss.at[k], grad_rs.at[k], own, there)

    for j in range(seqs // half):
        turned = dkv_acc[:, j * TILE : (j + 1) * TILE].T
        for i in range(half):
            at = i * packed
            piece = jnp.concatenate([turned[at : at + packed], turned[at + HALF : at + HALF + packed]], axis=0)
            grad_send[j * half + i] = piece.astype(BF16)
    for k in range(1, seqs):
        grad_copy(k).start()
    grad_recv[0] = grad_send[seq]

    for g in range(seqs):
        remote_here = jnp.logical_or(unit != 0, seq != g)

        @pl.when(remote_here)
        def _():
            dq_arrival(g).wait_recv()

    for i in range(seqs // 2):
        at = 3 * LANES * i
        qg_out[0, :, at : at + LANES] = dq_recv[2 * i, 0]
        both = jnp.where(low, dq_recv[2 * i, 1].astype(F32), dq_recv[2 * i + 1, 0].astype(F32))
        qg_out[0, :, at + LANES : at + 2 * LANES] = both.astype(BF16)
        qg_out[0, :, at + 2 * LANES : at + 3 * LANES] = dq_recv[2 * i + 1, 1]

    for k in range(1, seqs):
        grad_copy(k).wait_recv()
    for i in range(seqs // 2):
        a = grad_recv[lax.rem(seq + seqs - 2 * i, seqs)]
        b = grad_recv[lax.rem(seq + seqs - 2 * i - 1, seqs)]
        key_part, value_part = paired(a.astype(F32), b.astype(F32))
        kg_out[0, :, i * LANES : (i + 1) * LANES] = key_part
        vg_out[0, :, i * LANES : (i + 1) * LANES] = value_part

    for k in range(1, seqs):
        for copy in (k_copy, v_copy, q_copy, do_copy, delta_copy, grad_copy):
            copy(k).wait_send()

    @pl.when(unit != 0)
    def _():
        for copy in (q_copy, do_copy, delta_copy):
            copy(0).wait_send()

    for j in range(seqs):
        if j < half:
            @pl.when(seq != j)
            def _():
                dq_copy(j).wait_send()
        else:
            dq_copy(j).wait_send()

    @pl.loop(1, spans)
    def _(k):
        @pl.when(needs(shifted(k, 1), own))
        def _():
            k_cast(k).wait_send()
            v_cast(k).wait_send()

        @pl.when(needs(own, shifted(k, -1)))
        def _():
            part_copy(k).wait_send()


def solution(mesh):
    seqs, spans = mesh.shape["seq"], mesh.shape["span"]
    spec = P("span", "seq", None)

    def per_device(queries, keys, values, attn_output, out_grad):
        tokens = queries.shape[1]
        block_len = tokens * seqs
        total = block_len * spans
        rows = QUERY_PER_KEY * TILE
        vmem = pl.BlockSpec(memory_space=pltpu.VMEM)
        dma = pltpu.SemaphoreType.DMA
        return pl.pallas_call(
            functools.partial(fused_kernel, seqs, spans),
            out_shape=(
                jax.ShapeDtypeStruct(queries.shape, BF16),
                jax.ShapeDtypeStruct(keys.shape, BF16),
                jax.ShapeDtypeStruct(values.shape, BF16),
            ),
            in_specs=[vmem] * 5,
            out_specs=(vmem,) * 3,
            scratch_shapes=[
                pltpu.VMEM((total // 2, LANES), BF16),
                pltpu.VMEM((total // 2, LANES), BF16),
                pltpu.VMEM((2, QUERY_PER_KEY, HALF, LANES), BF16),
                pltpu.VMEM((2, QUERY_PER_KEY, HALF, LANES), BF16),
                pltpu.VMEM((2, seqs // 2, 8, tokens), F32),
                pltpu.VMEM((2, 256, rows), BF16),
                pltpu.VMEM((2, QUERY_PER_KEY, TILE, LANES), BF16),
                pltpu.VMEM((2, QUERY_PER_KEY, TILE, LANES), BF16),
                pltpu.VMEM((total, LANES), BF16),
                pltpu.VMEM((256, total), BF16),
                pltpu.VMEM((256, total), BF16),
                pltpu.VMEM((2 * TILE, 256), BF16),
                pltpu.VMEM((2, 8, rows), F32),
                pltpu.VMEM((2, 8, rows), F32),
                pltpu.VMEM((2, rows, LANES), F32),
                pltpu.VMEM((rows, TILE), BF16),
                pltpu.VMEM((rows, TILE), BF16),
                pltpu.VMEM((LANES, block_len), F32),
                pltpu.VMEM((seqs, tokens // 2, LANES), BF16),
                pltpu.VMEM((seqs, tokens // 2, LANES), BF16),
                pltpu.VMEM((seqs, QUERY_PER_KEY, tokens // 2, LANES), BF16),
                pltpu.VMEM((seqs, QUERY_PER_KEY, tokens // 2, LANES), BF16),
                pltpu.VMEM((8 * seqs, tokens), F32),
                pltpu.VMEM((spans, LANES, block_len), BF16),
                pltpu.VMEM((spans, LANES, block_len), BF16),
                pltpu.VMEM((seqs, 2, tokens, LANES), BF16),
                pltpu.VMEM((seqs, 2, tokens, LANES), BF16),
                pltpu.VMEM((seqs, tokens, LANES), BF16),
                pltpu.VMEM((seqs, tokens, LANES), BF16),
            ]
            + [dma((seqs,))] * 10 + [dma((spans,))] * 6 + [dma((seqs,))] * 4,
            compiler_params=pltpu.CompilerParams(
                vmem_limit_bytes=60 * 1024 * 1024, collective_id=0, has_side_effects=True
            ),
            name="attention_grads",
        )(queries, keys, values, attn_output, out_grad)

    return jax.shard_map(
        per_device, mesh=mesh, in_specs=(spec,) * 5, out_specs=(spec,) * 3, check_vma=False
    )
```

```python
import functools
import math

import jax
import jax.numpy as jnp
from jax import lax
from jax.experimental import pallas as pl
from jax.experimental.pallas import tpu as pltpu
from jax.sharding import PartitionSpec as P

HEAD_WIDTH = 64
QUERY_PER_KEY = 3
TILE = 512
HALF = TILE // 2
VALUES_AT = 4
PLACES = (
    (0, 0), (2, 0), (2, 1), (2, 3), (2, 2), (3, 2), (0, 2), (1, 2),
    (1, 1), (3, 0), (0, 3), (3, 3), (1, 0), (1, 3), (3, 1), (0, 1),
)
VIA = {(2, 2): (1, 2), (2, 0): (1, 0), (2, 1): (3, 1), (2, 3): (3, 3), (1, 2): (1, 3), (3, 2): (3, 1), (0, 2): (0, 1)}
LAST_RELAYED = 7
KEYS_ON = ((1, 15), (2, 14), (3, 13), (3, 12), (3, 11), (6, 7))
VALUES_ON = ((12, 15), (12, 14), (12, 13), (12, 12), (12, 11), (14, 7))
STRIP = 64
LANES = 128
NEG_LARGE = -1e30
SCORE_SCALE = 1.0 / math.sqrt(HEAD_WIDTH)
BASE2_SCALE = SCORE_SCALE * math.log2(math.e)
F32 = jnp.float32
BF16 = jnp.bfloat16


def dot(a, b, contract):
    return lax.dot_general(a, b, ((contract[0], contract[1]), ((), ())), preferred_element_type=F32)


def three_parts(x):
    first = x.astype(BF16).astype(F32)
    rest = x - first
    second = rest.astype(BF16).astype(F32)
    return first, second, rest - second


def fused_kernel(seqs, spans, q_in, k_in, v_in, o_in, do_in, qg_out, kg_out, vg_out, k_got, v_got, q_got, do_got, delta, lt, l1, l2, k_rows,
                 ks_t, vs_t, ks, s_buf, stat_m, stat_l, dq_acc, p_buf, ds_buf, dkv_acc, k_send, v_send, q_send, do_send, delta_send,
                 part_send, part_recv, dq_send, dq_recv, grad_send, grad_recv, k_ss, k_rs, v_ss, v_rs, q_ss, q_rs, do_ss, do_rs,
                 delta_ss, delta_rs, kcast_ss, kcast_rs, vcast_ss, vcast_rs, part_ss, part_rs, dq_ss, dq_rs, grad_ss, grad_rs):
    own = lax.axis_index("span")
    seq = lax.axis_index("seq")
    tokens = q_in.shape[1]
    block_len = tokens * seqs
    half = seqs // 2
    rows = QUERY_PER_KEY * TILE
    key_tiles = k_rows.shape[0] // TILE
    packed = tokens // 2
    mirror = spans - 1 - own
    unit = lax.div(seq, half)
    unit_span = jnp.where(unit == 0, own, mirror)
    unit_piece = lax.rem(seq, half)

    def needs(span, block):
        return block <= jnp.maximum(span, spans - 1 - span)

    def entry(values, k):
        found = values[0] + 0 * k
        for i, value in enumerate(values):
            if value != values[0]:
                found = jnp.where(k == i, value, found)
        return found

    def moved(x_step, z_step):
        x = lax.rem(lax.div(own, 4) + 4 + x_step, 4)
        z = lax.rem(lax.rem(own, 4) + 4 + z_step, 4)
        return x * 4 + z

    def shifted(k, sign):
        return moved(sign * entry([p[0] for p in PLACES], k), sign * entry([p[1] for p in PLACES], k))

    def next_place(p):
        return VIA.get(p, (0, 0))

    def place_before(k):
        steps = [[(next_place(p)[axis] - p[axis] + 4) % 4 for p in PLACES] for axis in range(2)]
        return moved(entry(steps[0], k), entry(steps[1], k))

    def place_after(k):
        steps = [[(next_place(p)[axis] - p[axis] + 4) % 4 for p in PLACES] for axis in range(2)]
        return moved(-entry(steps[0], k), -entry(steps[1], k))

    joins = [[PLACES.index(c) for c in PLACES if VIA.get(c) == p] for p in PLACES]

    def joining(k, i):
        return entry([c[i] if len(c) > i else 0 for c in joins], k)

    def seq_shifted(k, sign):
        return lax.rem(seq + seqs + sign * k, seqs)

    def remote(source, target, send, receive, span, at_seq):
        return pltpu.make_async_remote_copy(
            src_ref=source, dst_ref=target, send_sem=send, recv_sem=receive,
            device_id={"span": span, "seq": at_seq}, device_id_type=pl.DeviceIdType.MESH,
        )

    barrier = pltpu.get_barrier_semaphore()

    def greet(span, at_seq):
        pl.semaphore_signal(barrier, inc=1, device_id={"span": span, "seq": at_seq}, device_id_type=pl.DeviceIdType.MESH)

    for k in range(1, seqs):
        greet(own, seq_shifted(k, 1))
    for k in range(seqs):
        greet(mirror, seq_shifted(k, 1))

    @pl.loop(1, spans)
    def _(k):
        there = shifted(k, 1)

        @pl.when(there != mirror)
        def _():
            greet(there, seq)

    def paired(a, b):
        mask = lax.broadcasted_iota(jnp.int32, a.shape, 1) < HEAD_WIDTH
        return (
            jnp.where(mask, a, pltpu.roll(b, HEAD_WIDTH, 1)).astype(BF16),
            jnp.where(mask, pltpu.roll(a, HEAD_WIDTH, 1), b).astype(BF16),
        )

    def pack(ref, i):
        at = slice(i * LANES, (i + 1) * LANES)
        return paired(ref[0, :packed, at].astype(F32), ref[0, packed:, at].astype(F32))

    heads = seqs * QUERY_PER_KEY

    def pack_keys(ref, out):
        for i in range(seqs // 2):
            out[2 * i], out[2 * i + 1] = pack(ref, i)

    def pack_queries(ref, out):
        for i in range(heads // 2):
            a, b = pack(ref, i)
            n = 2 * i
            out[n // QUERY_PER_KEY, n % QUERY_PER_KEY] = a
            n = 2 * i + 1
            out[n // QUERY_PER_KEY, n % QUERY_PER_KEY] = b

    pack_keys(k_in, k_send)
    pl.semaphore_wait(barrier, (seqs - 1) + seqs + (spans - 2))

    own_rows = pl.ds(pl.multiple_of(own * (block_len // 2) + seq * packed, packed), packed)
    unit_rows = pl.ds(pl.multiple_of(unit_piece * packed, packed), packed)

    def k_copy(k):
        there = seq_shifted(k, 1)
        return remote(k_send.at[there], k_got.at[own_rows], k_ss.at[k], k_rs.at[k], own, there)

    def v_copy(k):
        there = seq_shifted(k, 1)
        return remote(v_send.at[there], v_got.at[own_rows], v_ss.at[k], v_rs.at[k], own, there)

    def q_copy(k):
        there = seq_shifted(k, 1)
        return remote(q_send.at[there], q_got.at[unit, :, unit_rows, :], q_ss.at[k], q_rs.at[k], unit_span, there)

    def do_copy(k):
        there = seq_shifted(k, 1)
        return remote(do_send.at[there], do_got.at[unit, :, unit_rows, :], do_ss.at[k], do_rs.at[k], unit_span, there)

    def delta_copy(k):
        there = seq_shifted(k, 1)
        return remote(
            delta_send.at[pl.ds(pl.multiple_of(there * 8, 8), 8), :], delta.at[unit, unit_piece],
            delta_ss.at[k], delta_rs.at[k], unit_span, there,
        )

    def block_rows(block):
        return pl.ds(pl.multiple_of(block * (block_len // 2), block_len // 2), block_len // 2)

    def cast_copy(k, got, send, receive):
        before = entry([PLACES.index(next_place(p)) for p in PLACES], k)
        at = block_rows(shifted(before, -1))
        return remote(got.at[at], got.at[at], send.at[k], receive.at[k], place_after(k), seq)

    def k_cast(k):
        return cast_copy(k, k_got, kcast_ss, kcast_rs)

    def v_cast(k):
        return cast_copy(k, v_got, vcast_ss, vcast_rs)

    def pass_on(k, cast):
        for i in range(max(len(c) for c in joins)):
            joined = joining(k, i)

            @pl.when(joined > 0)
            def _():
                cast(joined).start()

    def cast_all(cast):
        @pl.loop(1, spans - LAST_RELAYED)
        def _(i):
            cast(spans - i).start()

    for k in range(1, seqs):
        k_copy(k).start()
    k_got[own_rows, :] = k_send[seq]
    pack_queries(q_in, q_send)
    for k in range(1, seqs):
        q_copy(k).start()

    @pl.when(unit == 0)
    def _():
        q_got[0, :, unit_rows, :] = q_send[seq]

    @pl.when(unit != 0)
    def _():
        q_copy(0).start()

    for k in range(1, seqs):
        k_copy(k).wait_recv()
    cast_all(k_cast)

    pack_keys(v_in, v_send)
    pack_queries(do_in, do_send)

    head_row = lax.broadcasted_iota(jnp.int32, (8 * seqs, heads * HEAD_WIDTH), 0)
    head_col = lax.broadcasted_iota(jnp.int32, (8 * seqs, heads * HEAD_WIDTH), 1)
    in_group = head_row - lax.shift_left(lax.shift_right_logical(head_row, 3), 3)
    wanted = lax.shift_right_logical(head_row, 3) * QUERY_PER_KEY + in_group
    member = (in_group < QUERY_PER_KEY) & (wanted == lax.shift_right_logical(head_col, 6))
    selector = jnp.where(member, 1.0, 0.0).astype(BF16)
    product = do_in[0].astype(F32) * o_in[0].astype(F32)
    product_high = product.astype(BF16)
    product_low = (product - product_high.astype(F32)).astype(BF16)
    delta_send[...] = dot(selector, product_high, ((1,), (1,))) + dot(selector, product_low, ((1,), (1,)))
    v_got[own_rows, :] = v_send[seq]

    @pl.when(unit == 0)
    def _():
        do_got[0, :, unit_rows, :] = do_send[seq]
        delta[0, unit_piece] = delta_send[pl.ds(pl.multiple_of(seq * 8, 8), 8), :]

    def from_everyone(copies):
        for k in range(1, seqs):
            copies(k).wait_recv()

        @pl.when(unit != 0)
        def _():
            copies(0).wait_recv()

    from_everyone(q_copy)

    def halves(x):
        return jnp.concatenate([x[0:HEAD_WIDTH], x[HEAD_WIDTH:]], axis=1)

    @pl.loop(0, 2)
    def _(u):
        for h in range(QUERY_PER_KEY):
            cols = pl.ds(h * TILE, TILE)
            turned = halves(q_got[u, h].astype(F32).T).astype(BF16)
            nothing = jnp.zeros((HEAD_WIDTH, TILE), BF16)
            lt[u, 0:64, cols] = turned
            lt[u, 64:128, cols] = nothing
            lt[u, 128:192, cols] = turned
            lt[u, 192:256, cols] = nothing
        dq_acc[u] = jnp.zeros((rows, LANES), F32)
        stat_m[u] = jnp.full((8, rows), NEG_LARGE, F32)
        stat_l[u] = jnp.zeros((8, rows), F32)

    aux_row = lax.broadcasted_iota(jnp.int32, (HEAD_WIDTH, TILE), 0)
    aux_s = jnp.where(aux_row < 3, -1.0, 0.0)
    aux_v = jnp.where((aux_row >= 3) & (aux_row < 6), -1.0, 0.0)

    def packed_tile(got, t):
        return got[pl.ds(pl.multiple_of(t * HALF, HALF), HALF), :].astype(F32)

    def prepare_keys(t):
        at = pl.ds(pl.multiple_of(t * TILE, TILE), TILE)
        raw = packed_tile(k_got, t)
        zero = jnp.zeros((HALF, LANES), F32)
        mask = lax.broadcasted_iota(jnp.int32, (HALF, LANES), 1) < HEAD_WIDTH

        def spread(x):
            return jnp.concatenate([jnp.where(mask, x, zero), jnp.where(mask, pltpu.roll(x, HEAD_WIDTH, 1), zero)], axis=0)

        scaled = raw * BASE2_SCALE
        high = scaled.astype(BF16).astype(F32)
        within = pl.ds(pl.multiple_of(lax.rem(t, 2) * TILE, TILE), TILE)
        ks[within, 0:128] = spread(high).astype(BF16)
        ks[within, 128:256] = spread(scaled - high).astype(BF16)
        nothing = jnp.zeros((HEAD_WIDTH, TILE), F32)
        turned = halves(raw.T)
        k_rows[at, :] = spread(raw).astype(BF16)
        scaled = turned * BASE2_SCALE
        high = scaled.astype(BF16).astype(F32)
        ks_t[0:128, at] = jnp.concatenate([high, nothing], axis=0).astype(BF16)
        ks_t[128:256, at] = jnp.concatenate([scaled - high, aux_s], axis=0).astype(BF16)

    def prepare_values(t):
        at = pl.ds(pl.multiple_of(t * TILE, TILE), TILE)
        nothing = jnp.zeros((HEAD_WIDTH, TILE), F32)
        vs_t[0:128, at] = jnp.concatenate([nothing, halves(packed_tile(v_got, t).T)], axis=0).astype(BF16)
        vs_t[128:256, at] = jnp.concatenate([nothing, aux_v], axis=0).astype(BF16)

    def place(axis):
        r = lax.broadcasted_iota(jnp.int32, (TILE, TILE), axis)
        quarter = lax.shift_right_logical(r & (HALF - 1), 6)
        return quarter * 128 + lax.shift_right_logical(r, 8) * 64 + (r & 63)

    def stats(u, t, masked):
        w = ks[pl.ds(pl.multiple_of(lax.rem(t, 2) * TILE, TILE), TILE), :]
        news = []

        def scores(h):
            cols = pl.ds(h * TILE, TILE)
            s = dot(w, lt[u, :, cols], ((1,), (0,)))
            if masked:
                s = jnp.where(place(0) <= place(1), s, NEG_LARGE)
            top = jnp.full((8, TILE), NEG_LARGE, F32)
            for r in range(0, TILE, STRIP):
                strip = s[r : r + STRIP]
                s_buf[h, r : r + STRIP, :] = strip
                for i in range(0, STRIP, 8):
                    top = jnp.maximum(top, strip[i : i + 8])
            news.append(jnp.maximum(stat_m[u, 0:1, cols], jnp.max(top, axis=0, keepdims=True)))

        def sums(h):
            cols = pl.ds(h * TILE, TILE)
            new = jnp.broadcast_to(news[h], (8, TILE))
            total = stat_l[u, :, cols] * jnp.exp2(stat_m[u, :, cols] - new)
            for r in range(0, TILE, 8):
                total = total + jnp.exp2(s_buf[h, r : r + 8, :] - new)
            stat_l[u, :, cols] = total
            stat_m[u, :, cols] = new

        scores(0)
        for h in range(1, QUERY_PER_KEY):
            scores(h)
            sums(h - 1)
        sums(QUERY_PER_KEY - 1)

    def visit(block, step, both=True, only=0):
        @pl.loop(0, 4)
        def _(i):
            u = lax.rem(i, 2)
            t = block * 2 + lax.div(i, 2)
            last = jnp.where(u == 0, 2 * own, key_tiles - 1 - 2 * own)
            wanted = jnp.logical_or(both, u == only)

            @pl.when(jnp.logical_and(wanted, t < last))
            def _():
                step(u, t, False)

            @pl.when(jnp.logical_and(wanted, t == last))
            def _():
                step(u, t, True)

    def arrives(k):
        return jnp.logical_and(k > 0, jnp.logical_and(k < 11, k != 7))

    def cast_wait(k, got, send, receive):
        at = block_rows(shifted(k, -1))
        remote(got.at[at], got.at[at], send.at[k], receive.at[k], place_before(k), seq).wait_recv()

    @pl.loop(0, spans)
    def _(step):
        k = lax.rem(spans - step, spans)
        block = shifted(k, -1)

        for at_step, on in KEYS_ON:
            @pl.when(step == at_step)
            def _():
                cast_wait(on, k_got, kcast_ss, kcast_rs)
                pass_on(on, k_cast)

        @pl.when(arrives(k))
        def _():
            cast_wait(k, k_got, kcast_ss, kcast_rs)

        @pl.when(needs(own, block))
        def _():
            prepare_keys(2 * block)
            prepare_keys(2 * block + 1)
            visit(block, stats)

        @pl.when(k == 0)
        def _():
            for copy in (v_copy, do_copy, delta_copy):
                for i in range(1, seqs):
                    copy(i).start()

            @pl.when(unit != 0)
            def _():
                do_copy(0).start()
                delta_copy(0).start()

        @pl.when(step == VALUES_AT)
        def _():
            for i in range(1, seqs):
                v_copy(i).wait_recv()
            cast_all(v_cast)

        for at_step, on in VALUES_ON:
            @pl.when(step == at_step)
            def _():
                cast_wait(on, v_got, vcast_ss, vcast_rs)
                pass_on(on, v_cast)

    from_everyone(delta_copy)
    from_everyone(do_copy)
    row = lax.broadcasted_iota(jnp.int32, (16, TILE), 0)

    @pl.loop(0, 2)
    def _(u):
        for h in range(QUERY_PER_KEY):
            cols = pl.ds(h * TILE, TILE)
            total = jnp.sum(stat_l[u, :, cols], axis=0, keepdims=True)
            lse = stat_m[u, 0:1, cols] + jnp.log2(total)
            pieces = [delta[u, i, h : h + 1, :] for i in range(half)]
            shifts = jnp.concatenate([x[:, :packed] for x in pieces] + [x[:, packed:] for x in pieces], axis=1)
            parts = three_parts(lse) + three_parts(shifts)
            block = jnp.zeros((16, TILE), F32)
            for i, part in enumerate(parts):
                block = jnp.where(row == i, part, block)
            lt[u, 192:208, cols] = block.astype(BF16)
            lt[u, 64:128, cols] = halves(do_got[u, h].astype(F32).T).astype(BF16)
            l1[u, h, :HALF, :], l1[u, h, HALF:, :] = paired(q_got[u, h].astype(F32), do_got[u, h].astype(F32))
            l2[u, h] = lt[u, 128:256, cols].astype(F32).T.astype(BF16)

    def main(u, t, masked):
        slot = jnp.where(lax.div(t, 2) == own, 1, 0)
        at = pl.ds(pl.multiple_of(t * TILE, TILE), TILE)
        within = pl.ds(pl.multiple_of(lax.rem(t, 2) * TILE, TILE), TILE)
        kw = ks_t[:, at]
        vw = vs_t[:, at]
        kr = k_rows[at, :]

        def products(h):
            lhs = jnp.concatenate([l1[u, h], l2[u, h]], axis=1)
            return dot(lhs, kw, ((1,), (0,))), dot(lhs, vw, ((1,), (0,)))

        def weights(h, s, dp):
            for r in range(0, TILE, STRIP):
                here = pl.ds(h * TILE + r, STRIP)
                p = jnp.exp2(s[r : r + STRIP])
                if masked:
                    p = jnp.where(place(1)[r : r + STRIP] <= place(0)[r : r + STRIP], p, 0.0)
                p_buf[here, :] = p.astype(BF16)
                ds_buf[here, :] = (p * dp[r : r + STRIP]).astype(BF16)

        for h in range(QUERY_PER_KEY):
            weights(h, *products(h))
            here = pl.ds(h * TILE, TILE)
            dq_acc[u, here, :] += dot(ds_buf[here, :], kr, ((1,), (0,)))
        dkv_acc[slot, 0:64, within] += dot(lt[u, 0:64, :], ds_buf[...], ((1,), (0,)))
        dkv_acc[slot, 64:128, within] += dot(lt[u, 64:128, :], p_buf[...], ((1,), (0,)))

    def part_copy(k):
        return remote(part_send.at[k], part_recv.at[k], part_ss.at[k], part_rs.at[k], shifted(k, -1), seq)

    def dq_copy(j):
        u, i = j // half, j % half
        at_span = own if u == 0 else mirror
        at = pl.ds(i * packed, packed)
        return remote(dq_send.at[u, :, at, :], dq_recv.at[seq], dq_ss.at[j], dq_rs.at[seq], at_span, j)

    def dq_arrival(g):
        return remote(dq_send.at[0, :, pl.ds(0, packed), :], dq_recv.at[g], dq_ss.at[0], dq_rs.at[g], own, g)

    def dq_pack(u):
        mask = lax.broadcasted_iota(jnp.int32, (HALF, LANES), 1) < HEAD_WIDTH
        for h in range(QUERY_PER_KEY):
            first = dq_acc[u, h * TILE : h * TILE + HALF, :]
            second = dq_acc[u, h * TILE + HALF : (h + 1) * TILE, :]
            dq_send[u, h] = (jnp.where(mask, first, pltpu.roll(second, HEAD_WIDTH, 1)) * SCORE_SCALE).astype(BF16)

    last_second = 0 * own
    for k in range(1, spans):
        last_second = jnp.where(shifted(k, -1) <= mirror, k, last_second)
    dkv_acc[1] = jnp.zeros((LANES, block_len), F32)

    @pl.loop(0, spans + 1)
    def _(j):
        k = lax.rem(j, spans)
        block = shifted(k, -1)

        @pl.when(arrives(k))
        def _():
            cast_wait(k, v_got, vcast_ss, vcast_rs)

        @pl.when(needs(own, block))
        def _():
            @pl.when(k > 0)
            def _():
                dkv_acc[0] = jnp.zeros((LANES, block_len), F32)

            @pl.when(j < spans)
            def _():
                prepare_values(2 * block)
                prepare_values(2 * block + 1)

            visit(block, main, k > 0, jnp.where(j == 0, 1, 0))

            @pl.when(k > 0)
            def _():
                part_send[k, 0:64, :] = (dkv_acc[0, 0:64, :] * SCORE_SCALE).astype(BF16)
                part_send[k, 64:128, :] = dkv_acc[0, 64:128, :].astype(BF16)
                part_copy(k).start()

        @pl.when(j == last_second)
        def _():
            dq_pack(1)
            for i in range(half, seqs):
                dq_copy(i).start()

    dq_pack(0)
    for j in range(half):
        @pl.when(seq == j)
        def _():
            dq_recv[j] = dq_send[0, :, j * packed : (j + 1) * packed, :]

        @pl.when(seq != j)
        def _():
            dq_copy(j).start()

    dkv_acc[1, 0:64, :] = dkv_acc[1, 0:64, :] * SCORE_SCALE

    @pl.loop(1, spans)
    def _(k):
        @pl.when(needs(shifted(k, 1), own))
        def _():
            part_copy(k).wait_recv()
            dkv_acc[1] += part_recv[k].astype(F32)

    def grad_copy(k):
        there = seq_shifted(k, 1)
        return remote(grad_send.at[there], grad_recv.at[k], grad_ss.at[k], grad_rs.at[k], own, there)

    for j in range(seqs // half):
        turned = dkv_acc[1, :, j * TILE : (j + 1) * TILE].T
        for i in range(half):
            at = i * packed
            piece = jnp.concatenate([turned[at : at + packed], turned[at + HALF : at + HALF + packed]], axis=0)
            grad_send[j * half + i] = piece.astype(BF16)
    for k in range(1, seqs):
        grad_copy(k).start()
    grad_recv[0] = grad_send[seq]

    for g in range(seqs):
        remote_here = jnp.logical_or(unit != 0, seq != g)

        @pl.when(remote_here)
        def _():
            dq_arrival(g).wait_recv()

    for i in range(heads // 2):
        a, b = (dq_recv[n // QUERY_PER_KEY, n % QUERY_PER_KEY].astype(F32) for n in (2 * i, 2 * i + 1))
        at = slice(i * LANES, (i + 1) * LANES)
        qg_out[0, :packed, at], qg_out[0, packed:, at] = paired(a, b)

    for k in range(1, seqs):
        grad_copy(k).wait_recv()
    for i in range(seqs // 2):
        a = grad_recv[lax.rem(seq + seqs - 2 * i, seqs)]
        b = grad_recv[lax.rem(seq + seqs - 2 * i - 1, seqs)]
        key_part, value_part = paired(a.astype(F32), b.astype(F32))
        kg_out[0, :, i * LANES : (i + 1) * LANES] = key_part
        vg_out[0, :, i * LANES : (i + 1) * LANES] = value_part

    for k in range(1, seqs):
        for copy in (k_copy, v_copy, q_copy, do_copy, delta_copy, grad_copy):
            copy(k).wait_send()

    @pl.when(unit != 0)
    def _():
        for copy in (q_copy, do_copy, delta_copy):
            copy(0).wait_send()

    for j in range(seqs):
        if j < half:
            @pl.when(seq != j)
            def _():
                dq_copy(j).wait_send()
        else:
            dq_copy(j).wait_send()

    @pl.loop(1, spans)
    def _(k):
        k_cast(k).wait_send()
        v_cast(k).wait_send()

        @pl.when(needs(own, shifted(k, -1)))
        def _():
            part_copy(k).wait_send()


def solution(mesh):
    seqs, spans = mesh.shape["seq"], mesh.shape["span"]
    spec = P("span", "seq", None)

    def per_device(queries, keys, values, attn_output, out_grad):
        tokens = queries.shape[1]
        block_len = tokens * seqs
        total = block_len * spans
        rows = QUERY_PER_KEY * TILE
        vmem = pl.BlockSpec(memory_space=pltpu.VMEM)
        dma = pltpu.SemaphoreType.DMA
        return pl.pallas_call(
            functools.partial(fused_kernel, seqs, spans),
            out_shape=(
                jax.ShapeDtypeStruct(queries.shape, BF16),
                jax.ShapeDtypeStruct(keys.shape, BF16),
                jax.ShapeDtypeStruct(values.shape, BF16),
            ),
            in_specs=[vmem] * 5,
            out_specs=(vmem,) * 3,
            scratch_shapes=[
                pltpu.VMEM((total // 2, LANES), BF16),
                pltpu.VMEM((total // 2, LANES), BF16),
                pltpu.VMEM((2, QUERY_PER_KEY, HALF, LANES), BF16),
                pltpu.VMEM((2, QUERY_PER_KEY, HALF, LANES), BF16),
                pltpu.VMEM((2, seqs // 2, 8, tokens), F32),
                pltpu.VMEM((2, 256, rows), BF16),
                pltpu.VMEM((2, QUERY_PER_KEY, TILE, LANES), BF16),
                pltpu.VMEM((2, QUERY_PER_KEY, TILE, LANES), BF16),
                pltpu.VMEM((total, LANES), BF16),
                pltpu.VMEM((256, total), BF16),
                pltpu.VMEM((256, total), BF16),
                pltpu.VMEM((2 * TILE, 256), BF16),
                pltpu.VMEM((QUERY_PER_KEY, TILE, TILE), F32),
                pltpu.VMEM((2, 8, rows), F32),
                pltpu.VMEM((2, 8, rows), F32),
                pltpu.VMEM((2, rows, LANES), F32),
                pltpu.VMEM((rows, TILE), BF16),
                pltpu.VMEM((rows, TILE), BF16),
                pltpu.VMEM((2, LANES, block_len), F32),
                pltpu.VMEM((seqs, tokens // 2, LANES), BF16),
                pltpu.VMEM((seqs, tokens // 2, LANES), BF16),
                pltpu.VMEM((seqs, QUERY_PER_KEY, tokens // 2, LANES), BF16),
                pltpu.VMEM((seqs, QUERY_PER_KEY, tokens // 2, LANES), BF16),
                pltpu.VMEM((8 * seqs, tokens), F32),
                pltpu.VMEM((spans, LANES, block_len), BF16),
                pltpu.VMEM((spans, LANES, block_len), BF16),
                pltpu.VMEM((2, QUERY_PER_KEY, HALF, LANES), BF16),
                pltpu.VMEM((seqs, QUERY_PER_KEY, tokens // 2, LANES), BF16),
                pltpu.VMEM((seqs, tokens, LANES), BF16),
                pltpu.VMEM((seqs, tokens, LANES), BF16),
            ]
            + [dma((seqs,))] * 10 + [dma((spans,))] * 6 + [dma((seqs,))] * 4,
            compiler_params=pltpu.CompilerParams(
                vmem_limit_bytes=60 * 1024 * 1024, collective_id=0, has_side_effects=True
            ),
            name="attention_grads",
        )(queries, keys, values, attn_output, out_grad)

    return jax.shard_map(
        per_device, mesh=mesh, in_specs=(spec,) * 5, out_specs=(spec,) * 3, check_vma=False
    )
```

```python
import functools
import math

import jax
import jax.numpy as jnp
from jax import lax
from jax.experimental import pallas as pl
from jax.experimental.pallas import tpu as pltpu
from jax.sharding import PartitionSpec as P

HEAD_WIDTH = 64
QUERY_PER_KEY = 3
TILE = 512
HALF = TILE // 2
VALUES_AT = 6
STRIP = 64
LANES = 128
NEG_LARGE = -1e30
SCORE_SCALE = 1.0 / math.sqrt(HEAD_WIDTH)
BASE2_SCALE = SCORE_SCALE * math.log2(math.e)
F32 = jnp.float32
BF16 = jnp.bfloat16


def dot(a, b, contract):
    return lax.dot_general(a, b, ((contract[0], contract[1]), ((), ())), preferred_element_type=F32)


def three_parts(x):
    first = x.astype(BF16).astype(F32)
    rest = x - first
    second = rest.astype(BF16).astype(F32)
    return first, second, rest - second


def fused_kernel(seqs, spans, q_in, k_in, v_in, o_in, do_in, qg_out, kg_out, vg_out, k_got, v_got, q_got, do_got, delta, lt, l1, l2, k_rows,
                 ks_t, vs_t, ks, s_buf, stat_m, stat_l, dq_acc, p_buf, ds_buf, dkv_acc, k_send, v_send, q_send, do_send, delta_send,
                 part_send, part_recv, dq_send, dq_recv, grad_send, grad_recv, k_ss, k_rs, v_ss, v_rs, q_ss, q_rs, do_ss, do_rs,
                 delta_ss, delta_rs, kcast_ss, kcast_rs, vcast_ss, vcast_rs, part_ss, part_rs, dq_ss, dq_rs, grad_ss, grad_rs):
    own = lax.axis_index("span")
    seq = lax.axis_index("seq")
    tokens = q_in.shape[1]
    block_len = tokens * seqs
    half = seqs // 2
    rows = QUERY_PER_KEY * TILE
    key_tiles = k_rows.shape[0] // TILE
    packed = tokens // 2
    mirror = spans - 1 - own
    unit = lax.div(seq, half)
    unit_span = jnp.where(unit == 0, own, mirror)
    unit_piece = lax.rem(seq, half)

    def needs(span, block):
        return block <= jnp.maximum(span, spans - 1 - span)

    def shifted(k, sign):
        z_step = lax.rem(k, 4)
        x_step = lax.rem(lax.div(k, 4) + z_step, 4)
        x = lax.rem(lax.div(own, 4) + 4 + sign * x_step, 4)
        z = lax.rem(lax.rem(own, 4) + 4 + sign * z_step, 4)
        return x * 4 + z

    def seq_shifted(k, sign):
        return lax.rem(seq + seqs + sign * k, seqs)

    def remote(source, target, send, receive, span, at_seq):
        return pltpu.make_async_remote_copy(
            src_ref=source, dst_ref=target, send_sem=send, recv_sem=receive,
            device_id={"span": span, "seq": at_seq}, device_id_type=pl.DeviceIdType.MESH,
        )

    barrier = pltpu.get_barrier_semaphore()

    def greet(span, at_seq):
        pl.semaphore_signal(barrier, inc=1, device_id={"span": span, "seq": at_seq}, device_id_type=pl.DeviceIdType.MESH)

    for k in range(1, seqs):
        greet(own, seq_shifted(k, 1))
    for k in range(seqs):
        greet(mirror, seq_shifted(k, 1))

    @pl.loop(1, spans)
    def _(k):
        there = shifted(k, 1)

        @pl.when(there != mirror)
        def _():
            greet(there, seq)

    def paired(a, b):
        mask = lax.broadcasted_iota(jnp.int32, a.shape, 1) < HEAD_WIDTH
        return (
            jnp.where(mask, a, pltpu.roll(b, HEAD_WIDTH, 1)).astype(BF16),
            jnp.where(mask, pltpu.roll(a, HEAD_WIDTH, 1), b).astype(BF16),
        )

    def pack(ref, i):
        at = slice(i * LANES, (i + 1) * LANES)
        return paired(ref[0, :packed, at].astype(F32), ref[0, packed:, at].astype(F32))

    heads = seqs * QUERY_PER_KEY

    def pack_keys(ref, out):
        for i in range(seqs // 2):
            out[2 * i], out[2 * i + 1] = pack(ref, i)

    def pack_queries(ref, out):
        for i in range(heads // 2):
            a, b = pack(ref, i)
            n = 2 * i
            out[n // QUERY_PER_KEY, n % QUERY_PER_KEY] = a
            n = 2 * i + 1
            out[n // QUERY_PER_KEY, n % QUERY_PER_KEY] = b

    pack_keys(k_in, k_send)
    pl.semaphore_wait(barrier, (seqs - 1) + seqs + (spans - 2))

    own_rows = pl.ds(pl.multiple_of(own * (block_len // 2) + seq * packed, packed), packed)
    unit_rows = pl.ds(pl.multiple_of(unit_piece * packed, packed), packed)

    def k_copy(k):
        there = seq_shifted(k, 1)
        return remote(k_send.at[there], k_got.at[own_rows], k_ss.at[k], k_rs.at[k], own, there)

    def v_copy(k):
        there = seq_shifted(k, 1)
        return remote(v_send.at[there], v_got.at[own_rows], v_ss.at[k], v_rs.at[k], own, there)

    def q_copy(k):
        there = seq_shifted(k, 1)
        return remote(q_send.at[there], q_got.at[unit, :, unit_rows, :], q_ss.at[k], q_rs.at[k], unit_span, there)

    def do_copy(k):
        there = seq_shifted(k, 1)
        return remote(do_send.at[there], do_got.at[unit, :, unit_rows, :], do_ss.at[k], do_rs.at[k], unit_span, there)

    def delta_copy(k):
        there = seq_shifted(k, 1)
        return remote(
            delta_send.at[pl.ds(pl.multiple_of(there * 8, 8), 8), :], delta.at[unit, unit_piece],
            delta_ss.at[k], delta_rs.at[k], unit_span, there,
        )

    def cast_copy(k, got, send, receive):
        at = pl.ds(pl.multiple_of(own * (block_len // 2), block_len // 2), block_len // 2)
        return remote(got.at[at], got.at[at], send.at[k], receive.at[k], shifted(k, 1), seq)

    def k_cast(k):
        return cast_copy(k, k_got, kcast_ss, kcast_rs)

    def v_cast(k):
        return cast_copy(k, v_got, vcast_ss, vcast_rs)

    def cast_all(cast):
        @pl.loop(1, spans)
        def _(k):
            @pl.when(needs(shifted(k, 1), own))
            def _():
                cast(k).start()

    for k in range(1, seqs):
        k_copy(k).start()
    k_got[own_rows, :] = k_send[seq]
    pack_queries(q_in, q_send)
    for k in range(1, seqs):
        q_copy(k).start()

    @pl.when(unit == 0)
    def _():
        q_got[0, :, unit_rows, :] = q_send[seq]

    @pl.when(unit != 0)
    def _():
        q_copy(0).start()

    for k in range(1, seqs):
        k_copy(k).wait_recv()
    cast_all(k_cast)

    pack_keys(v_in, v_send)
    pack_queries(do_in, do_send)

    head_row = lax.broadcasted_iota(jnp.int32, (8 * seqs, heads * HEAD_WIDTH), 0)
    head_col = lax.broadcasted_iota(jnp.int32, (8 * seqs, heads * HEAD_WIDTH), 1)
    in_group = head_row - lax.shift_left(lax.shift_right_logical(head_row, 3), 3)
    wanted = lax.shift_right_logical(head_row, 3) * QUERY_PER_KEY + in_group
    member = (in_group < QUERY_PER_KEY) & (wanted == lax.shift_right_logical(head_col, 6))
    selector = jnp.where(member, 1.0, 0.0).astype(BF16)
    product = do_in[0].astype(F32) * o_in[0].astype(F32)
    product_high = product.astype(BF16)
    product_low = (product - product_high.astype(F32)).astype(BF16)
    delta_send[...] = dot(selector, product_high, ((1,), (1,))) + dot(selector, product_low, ((1,), (1,)))
    v_got[own_rows, :] = v_send[seq]

    @pl.when(unit == 0)
    def _():
        do_got[0, :, unit_rows, :] = do_send[seq]
        delta[0, unit_piece] = delta_send[pl.ds(pl.multiple_of(seq * 8, 8), 8), :]

    def from_everyone(copies):
        for k in range(1, seqs):
            copies(k).wait_recv()

        @pl.when(unit != 0)
        def _():
            copies(0).wait_recv()

    from_everyone(q_copy)

    def halves(x):
        return jnp.concatenate([x[0:HEAD_WIDTH], x[HEAD_WIDTH:]], axis=1)

    @pl.loop(0, 2)
    def _(u):
        for h in range(QUERY_PER_KEY):
            cols = pl.ds(h * TILE, TILE)
            turned = halves(q_got[u, h].astype(F32).T).astype(BF16)
            nothing = jnp.zeros((HEAD_WIDTH, TILE), BF16)
            lt[u, 0:64, cols] = turned
            lt[u, 64:128, cols] = nothing
            lt[u, 128:192, cols] = turned
            lt[u, 192:256, cols] = nothing
        dq_acc[u] = jnp.zeros((rows, LANES), F32)
        stat_m[u] = jnp.full((8, rows), NEG_LARGE, F32)
        stat_l[u] = jnp.zeros((8, rows), F32)

    aux_row = lax.broadcasted_iota(jnp.int32, (HEAD_WIDTH, TILE), 0)
    aux_s = jnp.where(aux_row < 3, -1.0, 0.0)
    aux_v = jnp.where((aux_row >= 3) & (aux_row < 6), -1.0, 0.0)

    def packed_tile(got, t):
        return got[pl.ds(pl.multiple_of(t * HALF, HALF), HALF), :].astype(F32)

    def prepare_keys(t):
        at = pl.ds(pl.multiple_of(t * TILE, TILE), TILE)
        raw = packed_tile(k_got, t)
        zero = jnp.zeros((HALF, LANES), F32)
        mask = lax.broadcasted_iota(jnp.int32, (HALF, LANES), 1) < HEAD_WIDTH

        def spread(x):
            return jnp.concatenate([jnp.where(mask, x, zero), jnp.where(mask, pltpu.roll(x, HEAD_WIDTH, 1), zero)], axis=0)

        scaled = raw * BASE2_SCALE
        high = scaled.astype(BF16).astype(F32)
        within = pl.ds(pl.multiple_of(lax.rem(t, 2) * TILE, TILE), TILE)
        ks[within, 0:128] = spread(high).astype(BF16)
        ks[within, 128:256] = spread(scaled - high).astype(BF16)
        nothing = jnp.zeros((HEAD_WIDTH, TILE), F32)
        turned = halves(raw.T)
        k_rows[at, :] = spread(raw).astype(BF16)
        scaled = turned * BASE2_SCALE
        high = scaled.astype(BF16).astype(F32)
        ks_t[0:128, at] = jnp.concatenate([high, nothing], axis=0).astype(BF16)
        ks_t[128:256, at] = jnp.concatenate([scaled - high, aux_s], axis=0).astype(BF16)

    def prepare_values(t):
        at = pl.ds(pl.multiple_of(t * TILE, TILE), TILE)
        nothing = jnp.zeros((HEAD_WIDTH, TILE), F32)
        vs_t[0:128, at] = jnp.concatenate([nothing, halves(packed_tile(v_got, t).T)], axis=0).astype(BF16)
        vs_t[128:256, at] = jnp.concatenate([nothing, aux_v], axis=0).astype(BF16)

    def place(axis):
        r = lax.broadcasted_iota(jnp.int32, (TILE, TILE), axis)
        quarter = lax.shift_right_logical(r & (HALF - 1), 6)
        return quarter * 128 + lax.shift_right_logical(r, 8) * 64 + (r & 63)

    def stats(u, t, masked):
        w = ks[pl.ds(pl.multiple_of(lax.rem(t, 2) * TILE, TILE), TILE), :]
        news = []

        def scores(h):
            cols = pl.ds(h * TILE, TILE)
            s = dot(w, lt[u, :, cols], ((1,), (0,)))
            if masked:
                s = jnp.where(place(0) <= place(1), s, NEG_LARGE)
            top = jnp.full((8, TILE), NEG_LARGE, F32)
            for r in range(0, TILE, STRIP):
                strip = s[r : r + STRIP]
                s_buf[h, r : r + STRIP, :] = strip
                for i in range(0, STRIP, 8):
                    top = jnp.maximum(top, strip[i : i + 8])
            news.append(jnp.maximum(stat_m[u, 0:1, cols], jnp.max(top, axis=0, keepdims=True)))

        def sums(h):
            cols = pl.ds(h * TILE, TILE)
            new = jnp.broadcast_to(news[h], (8, TILE))
            total = stat_l[u, :, cols] * jnp.exp2(stat_m[u, :, cols] - new)
            for r in range(0, TILE, 8):
                total = total + jnp.exp2(s_buf[h, r : r + 8, :] - new)
            stat_l[u, :, cols] = total
            stat_m[u, :, cols] = new

        scores(0)
        for h in range(1, QUERY_PER_KEY):
            scores(h)
            sums(h - 1)
        sums(QUERY_PER_KEY - 1)

    def visit(block, step):
        @pl.loop(0, 4)
        def _(i):
            u = lax.rem(i, 2)
            t = block * 2 + lax.div(i, 2)
            last = jnp.where(u == 0, 2 * own, key_tiles - 1 - 2 * own)

            @pl.when(t < last)
            def _():
                step(u, t, False)

            @pl.when(t == last)
            def _():
                step(u, t, True)

    def cast_wait(k, got, send, receive):
        at = pl.ds(pl.multiple_of(shifted(k, -1) * (block_len // 2), block_len // 2), block_len // 2)
        remote(got.at[at], got.at[at], send.at[k], receive.at[k], shifted(k, 1), seq).wait_recv()

    @pl.loop(0, spans)
    def _(k):
        block = shifted(k, -1)

        @pl.when(needs(own, block))
        def _():
            @pl.when(k > 0)
            def _():
                cast_wait(k, k_got, kcast_ss, kcast_rs)

            prepare_keys(2 * block)
            prepare_keys(2 * block + 1)
            visit(block, stats)

        @pl.when(k == 0)
        def _():
            for copy in (v_copy, do_copy, delta_copy):
                for i in range(1, seqs):
                    copy(i).start()

            @pl.when(unit != 0)
            def _():
                do_copy(0).start()
                delta_copy(0).start()

        @pl.when(k == VALUES_AT)
        def _():
            for i in range(1, seqs):
                v_copy(i).wait_recv()
            cast_all(v_cast)

    from_everyone(delta_copy)
    from_everyone(do_copy)
    row = lax.broadcasted_iota(jnp.int32, (16, TILE), 0)

    @pl.loop(0, 2)
    def _(u):
        for h in range(QUERY_PER_KEY):
            cols = pl.ds(h * TILE, TILE)
            total = jnp.sum(stat_l[u, :, cols], axis=0, keepdims=True)
            lse = stat_m[u, 0:1, cols] + jnp.log2(total)
            pieces = [delta[u, i, h : h + 1, :] for i in range(half)]
            shifts = jnp.concatenate([x[:, :packed] for x in pieces] + [x[:, packed:] for x in pieces], axis=1)
            parts = three_parts(lse) + three_parts(shifts)
            block = jnp.zeros((16, TILE), F32)
            for i, part in enumerate(parts):
                block = jnp.where(row == i, part, block)
            lt[u, 192:208, cols] = block.astype(BF16)
            lt[u, 64:128, cols] = halves(do_got[u, h].astype(F32).T).astype(BF16)
            l1[u, h, :HALF, :], l1[u, h, HALF:, :] = paired(q_got[u, h].astype(F32), do_got[u, h].astype(F32))
            l2[u, h] = lt[u, 128:256, cols].astype(F32).T.astype(BF16)

    def main(u, t, masked):
        at = pl.ds(pl.multiple_of(t * TILE, TILE), TILE)
        within = pl.ds(pl.multiple_of(lax.rem(t, 2) * TILE, TILE), TILE)
        kw = ks_t[:, at]
        vw = vs_t[:, at]
        kr = k_rows[at, :]

        def products(h):
            lhs = jnp.concatenate([l1[u, h], l2[u, h]], axis=1)
            return dot(lhs, kw, ((1,), (0,))), dot(lhs, vw, ((1,), (0,)))

        def weights(h, s, dp):
            for r in range(0, TILE, STRIP):
                here = pl.ds(h * TILE + r, STRIP)
                p = jnp.exp2(s[r : r + STRIP])
                if masked:
                    p = jnp.where(place(1)[r : r + STRIP] <= place(0)[r : r + STRIP], p, 0.0)
                p_buf[here, :] = p.astype(BF16)
                ds_buf[here, :] = (p * dp[r : r + STRIP]).astype(BF16)

        for h in range(QUERY_PER_KEY):
            weights(h, *products(h))
            here = pl.ds(h * TILE, TILE)
            dq_acc[u, here, :] += dot(ds_buf[here, :], kr, ((1,), (0,)))
        dkv_acc[0:64, within] += dot(lt[u, 0:64, :], ds_buf[...], ((1,), (0,)))
        dkv_acc[64:128, within] += dot(lt[u, 64:128, :], p_buf[...], ((1,), (0,)))

    def part_copy(k):
        return remote(part_send.at[k], part_recv.at[k], part_ss.at[k], part_rs.at[k], shifted(k, -1), seq)

    @pl.loop(1, spans + 1)
    def _(j):
        k = lax.rem(j, spans)
        block = shifted(k, -1)

        @pl.when(needs(own, block))
        def _():
            @pl.when(k > 0)
            def _():
                cast_wait(k, v_got, vcast_ss, vcast_rs)

            prepare_values(2 * block)
            prepare_values(2 * block + 1)
            dkv_acc[...] = jnp.zeros((LANES, block_len), F32)
            visit(block, main)
            dkv_acc[0:64, :] = dkv_acc[0:64, :] * SCORE_SCALE

            @pl.when(k > 0)
            def _():
                part_send[k] = dkv_acc[...].astype(BF16)
                part_copy(k).start()

    def dq_copy(j):
        u, i = j // half, j % half
        at_span = own if u == 0 else mirror
        at = pl.ds(i * packed, packed)
        return remote(dq_send.at[u, :, at, :], dq_recv.at[seq], dq_ss.at[j], dq_rs.at[seq], at_span, j)

    def dq_arrival(g):
        return remote(dq_send.at[0, :, pl.ds(0, packed), :], dq_recv.at[g], dq_ss.at[0], dq_rs.at[g], own, g)

    for u in (1, 0):
        for h in range(QUERY_PER_KEY):
            mask = lax.broadcasted_iota(jnp.int32, (HALF, LANES), 1) < HEAD_WIDTH
            first = dq_acc[u, h * TILE : h * TILE + HALF, :]
            second = dq_acc[u, h * TILE + HALF : (h + 1) * TILE, :]
            dq_send[u, h] = (jnp.where(mask, first, pltpu.roll(second, HEAD_WIDTH, 1)) * SCORE_SCALE).astype(BF16)
        for i in range(half):
            j = u * half + i
            if u == 0:
                @pl.when(seq == j)
                def _():
                    dq_recv[j] = dq_send[0, :, i * packed : (i + 1) * packed, :]

                @pl.when(seq != j)
                def _():
                    dq_copy(j).start()
            else:
                dq_copy(j).start()

    @pl.loop(1, spans)
    def _(k):
        @pl.when(needs(shifted(k, 1), own))
        def _():
            part_copy(k).wait_recv()
            dkv_acc[...] += part_recv[k].astype(F32)

    def grad_copy(k):
        there = seq_shifted(k, 1)
        return remote(grad_send.at[there], grad_recv.at[k], grad_ss.at[k], grad_rs.at[k], own, there)

    for j in range(seqs // half):
        turned = dkv_acc[:, j * TILE : (j + 1) * TILE].T
        for i in range(half):
            at = i * packed
            piece = jnp.concatenate([turned[at : at + packed], turned[at + HALF : at + HALF + packed]], axis=0)
            grad_send[j * half + i] = piece.astype(BF16)
    for k in range(1, seqs):
        grad_copy(k).start()
    grad_recv[0] = grad_send[seq]

    for g in range(seqs):
        remote_here = jnp.logical_or(unit != 0, seq != g)

        @pl.when(remote_here)
        def _():
            dq_arrival(g).wait_recv()

    for i in range(heads // 2):
        a, b = (dq_recv[n // QUERY_PER_KEY, n % QUERY_PER_KEY].astype(F32) for n in (2 * i, 2 * i + 1))
        at = slice(i * LANES, (i + 1) * LANES)
        qg_out[0, :packed, at], qg_out[0, packed:, at] = paired(a, b)

    for k in range(1, seqs):
        grad_copy(k).wait_recv()
    for i in range(seqs // 2):
        a = grad_recv[lax.rem(seq + seqs - 2 * i, seqs)]
        b = grad_recv[lax.rem(seq + seqs - 2 * i - 1, seqs)]
        key_part, value_part = paired(a.astype(F32), b.astype(F32))
        kg_out[0, :, i * LANES : (i + 1) * LANES] = key_part
        vg_out[0, :, i * LANES : (i + 1) * LANES] = value_part

    for k in range(1, seqs):
        for copy in (k_copy, v_copy, q_copy, do_copy, delta_copy, grad_copy):
            copy(k).wait_send()

    @pl.when(unit != 0)
    def _():
        for copy in (q_copy, do_copy, delta_copy):
            copy(0).wait_send()

    for j in range(seqs):
        if j < half:
            @pl.when(seq != j)
            def _():
                dq_copy(j).wait_send()
        else:
            dq_copy(j).wait_send()

    @pl.loop(1, spans)
    def _(k):
        @pl.when(needs(shifted(k, 1), own))
        def _():
            k_cast(k).wait_send()
            v_cast(k).wait_send()

        @pl.when(needs(own, shifted(k, -1)))
        def _():
            part_copy(k).wait_send()


def solution(mesh):
    seqs, spans = mesh.shape["seq"], mesh.shape["span"]
    spec = P("span", "seq", None)

    def per_device(queries, keys, values, attn_output, out_grad):
        tokens = queries.shape[1]
        block_len = tokens * seqs
        total = block_len * spans
        rows = QUERY_PER_KEY * TILE
        vmem = pl.BlockSpec(memory_space=pltpu.VMEM)
        dma = pltpu.SemaphoreType.DMA
        return pl.pallas_call(
            functools.partial(fused_kernel, seqs, spans),
            out_shape=(
                jax.ShapeDtypeStruct(queries.shape, BF16),
                jax.ShapeDtypeStruct(keys.shape, BF16),
                jax.ShapeDtypeStruct(values.shape, BF16),
            ),
            in_specs=[vmem] * 5,
            out_specs=(vmem,) * 3,
            scratch_shapes=[
                pltpu.VMEM((total // 2, LANES), BF16),
                pltpu.VMEM((total // 2, LANES), BF16),
                pltpu.VMEM((2, QUERY_PER_KEY, HALF, LANES), BF16),
                pltpu.VMEM((2, QUERY_PER_KEY, HALF, LANES), BF16),
                pltpu.VMEM((2, seqs // 2, 8, tokens), F32),
                pltpu.VMEM((2, 256, rows), BF16),
                pltpu.VMEM((2, QUERY_PER_KEY, TILE, LANES), BF16),
                pltpu.VMEM((2, QUERY_PER_KEY, TILE, LANES), BF16),
                pltpu.VMEM((total, LANES), BF16),
                pltpu.VMEM((256, total), BF16),
                pltpu.VMEM((256, total), BF16),
                pltpu.VMEM((2 * TILE, 256), BF16),
                pltpu.VMEM((QUERY_PER_KEY, TILE, TILE), F32),
                pltpu.VMEM((2, 8, rows), F32),
                pltpu.VMEM((2, 8, rows), F32),
                pltpu.VMEM((2, rows, LANES), F32),
                pltpu.VMEM((rows, TILE), BF16),
                pltpu.VMEM((rows, TILE), BF16),
                pltpu.VMEM((LANES, block_len), F32),
                pltpu.VMEM((seqs, tokens // 2, LANES), BF16),
                pltpu.VMEM((seqs, tokens // 2, LANES), BF16),
                pltpu.VMEM((seqs, QUERY_PER_KEY, tokens // 2, LANES), BF16),
                pltpu.VMEM((seqs, QUERY_PER_KEY, tokens // 2, LANES), BF16),
                pltpu.VMEM((8 * seqs, tokens), F32),
                pltpu.VMEM((spans, LANES, block_len), BF16),
                pltpu.VMEM((spans, LANES, block_len), BF16),
                pltpu.VMEM((2, QUERY_PER_KEY, HALF, LANES), BF16),
                pltpu.VMEM((seqs, QUERY_PER_KEY, tokens // 2, LANES), BF16),
                pltpu.VMEM((seqs, tokens, LANES), BF16),
                pltpu.VMEM((seqs, tokens, LANES), BF16),
            ]
            + [dma((seqs,))] * 10 + [dma((spans,))] * 6 + [dma((seqs,))] * 4,
            compiler_params=pltpu.CompilerParams(
                vmem_limit_bytes=60 * 1024 * 1024, collective_id=0, has_side_effects=True
            ),
            name="attention_grads",
        )(queries, keys, values, attn_output, out_grad)

    return jax.shard_map(
        per_device, mesh=mesh, in_specs=(spec,) * 5, out_specs=(spec,) * 3, check_vma=False
    )
```

```python
import functools
import math

import jax
import jax.numpy as jnp
from jax import lax
from jax.experimental import pallas as pl
from jax.experimental.pallas import tpu as pltpu
from jax.sharding import PartitionSpec as P

HEAD_WIDTH = 64
QUERY_PER_KEY = 3
TILE = 512
HALF = TILE // 2
VALUES_AT = 6
STRIP = 64
LANES = 128
NEG_LARGE = -1e30
SCORE_SCALE = 1.0 / math.sqrt(HEAD_WIDTH)
BASE2_SCALE = SCORE_SCALE * math.log2(math.e)
F32 = jnp.float32
BF16 = jnp.bfloat16


def dot(a, b, contract):
    return lax.dot_general(a, b, ((contract[0], contract[1]), ((), ())), preferred_element_type=F32)


def three_parts(x):
    first = x.astype(BF16).astype(F32)
    rest = x - first
    second = rest.astype(BF16).astype(F32)
    return first, second, rest - second


def fused_kernel(seqs, spans, q_in, k_in, v_in, o_in, do_in, qg_out, kg_out, vg_out, k_got, v_got, q_got, do_got, delta, lt, l1, l2, k_rows,
                 ks_t, vs_t, ks, s_buf, stat_m, stat_l, dq_acc, p_buf, ds_buf, dkv_acc, k_send, v_send, q_send, do_send, delta_send,
                 part_send, part_recv, dq_send, dq_recv, grad_send, grad_recv, k_ss, k_rs, v_ss, v_rs, q_ss, q_rs, do_ss, do_rs,
                 delta_ss, delta_rs, kcast_ss, kcast_rs, vcast_ss, vcast_rs, part_ss, part_rs, dq_ss, dq_rs, grad_ss, grad_rs):
    own = lax.axis_index("span")
    seq = lax.axis_index("seq")
    tokens = q_in.shape[1]
    block_len = tokens * seqs
    half = seqs // 2
    rows = QUERY_PER_KEY * TILE
    key_tiles = k_rows.shape[0] // TILE
    packed = tokens // 2
    mirror = spans - 1 - own
    unit = lax.div(seq, half)
    unit_span = jnp.where(unit == 0, own, mirror)
    unit_piece = lax.rem(seq, half)

    def needs(span, block):
        return block <= jnp.maximum(span, spans - 1 - span)

    def shifted(k, sign):
        z_step = lax.rem(k, 4)
        x_step = lax.rem(lax.div(k, 4) + z_step, 4)
        x = lax.rem(lax.div(own, 4) + 4 + sign * x_step, 4)
        z = lax.rem(lax.rem(own, 4) + 4 + sign * z_step, 4)
        return x * 4 + z

    def seq_shifted(k, sign):
        return lax.rem(seq + seqs + sign * k, seqs)

    def remote(source, target, send, receive, span, at_seq):
        return pltpu.make_async_remote_copy(
            src_ref=source, dst_ref=target, send_sem=send, recv_sem=receive,
            device_id={"span": span, "seq": at_seq}, device_id_type=pl.DeviceIdType.MESH,
        )

    barrier = pltpu.get_barrier_semaphore()

    def greet(span, at_seq):
        pl.semaphore_signal(barrier, inc=1, device_id={"span": span, "seq": at_seq}, device_id_type=pl.DeviceIdType.MESH)

    for k in range(1, seqs):
        greet(own, seq_shifted(k, 1))
    for k in range(seqs):
        greet(mirror, seq_shifted(k, 1))

    @pl.loop(1, spans)
    def _(k):
        there = shifted(k, 1)

        @pl.when(there != mirror)
        def _():
            greet(there, seq)

    def paired(a, b):
        mask = lax.broadcasted_iota(jnp.int32, a.shape, 1) < HEAD_WIDTH
        return (
            jnp.where(mask, a, pltpu.roll(b, HEAD_WIDTH, 1)).astype(BF16),
            jnp.where(mask, pltpu.roll(a, HEAD_WIDTH, 1), b).astype(BF16),
        )

    def pack(ref, i):
        at = slice(i * LANES, (i + 1) * LANES)
        return paired(ref[0, :packed, at].astype(F32), ref[0, packed:, at].astype(F32))

    heads = seqs * QUERY_PER_KEY

    def pack_keys(ref, out):
        for i in range(seqs // 2):
            out[2 * i], out[2 * i + 1] = pack(ref, i)

    def pack_queries(ref, out):
        for i in range(heads // 2):
            a, b = pack(ref, i)
            n = 2 * i
            out[n // QUERY_PER_KEY, n % QUERY_PER_KEY] = a
            n = 2 * i + 1
            out[n // QUERY_PER_KEY, n % QUERY_PER_KEY] = b

    pack_keys(k_in, k_send)
    pl.semaphore_wait(barrier, (seqs - 1) + seqs + (spans - 2))

    own_rows = pl.ds(pl.multiple_of(own * (block_len // 2) + seq * packed, packed), packed)
    unit_rows = pl.ds(pl.multiple_of(unit_piece * packed, packed), packed)

    def k_copy(k):
        there = seq_shifted(k, 1)
        return remote(k_send.at[there], k_got.at[own_rows], k_ss.at[k], k_rs.at[k], own, there)

    def v_copy(k):
        there = seq_shifted(k, 1)
        return remote(v_send.at[there], v_got.at[own_rows], v_ss.at[k], v_rs.at[k], own, there)

    def q_copy(k):
        there = seq_shifted(k, 1)
        return remote(q_send.at[there], q_got.at[unit, :, unit_rows, :], q_ss.at[k], q_rs.at[k], unit_span, there)

    def do_copy(k):
        there = seq_shifted(k, 1)
        return remote(do_send.at[there], do_got.at[unit, :, unit_rows, :], do_ss.at[k], do_rs.at[k], unit_span, there)

    def delta_copy(k):
        there = seq_shifted(k, 1)
        return remote(
            delta_send.at[pl.ds(pl.multiple_of(there * 8, 8), 8), :], delta.at[unit, unit_piece],
            delta_ss.at[k], delta_rs.at[k], unit_span, there,
        )

    def cast_copy(k, got, send, receive):
        at = pl.ds(pl.multiple_of(own * (block_len // 2), block_len // 2), block_len // 2)
        return remote(got.at[at], got.at[at], send.at[k], receive.at[k], shifted(k, 1), seq)

    def k_cast(k):
        return cast_copy(k, k_got, kcast_ss, kcast_rs)

    def v_cast(k):
        return cast_copy(k, v_got, vcast_ss, vcast_rs)

    def cast_all(cast):
        @pl.loop(1, spans)
        def _(k):
            @pl.when(needs(shifted(k, 1), own))
            def _():
                cast(k).start()

    for k in range(1, seqs):
        k_copy(k).start()
    k_got[own_rows, :] = k_send[seq]
    pack_queries(q_in, q_send)
    for k in range(1, seqs):
        q_copy(k).start()

    @pl.when(unit == 0)
    def _():
        q_got[0, :, unit_rows, :] = q_send[seq]

    @pl.when(unit != 0)
    def _():
        q_copy(0).start()

    for k in range(1, seqs):
        k_copy(k).wait_recv()
    cast_all(k_cast)

    pack_keys(v_in, v_send)
    pack_queries(do_in, do_send)

    head_row = lax.broadcasted_iota(jnp.int32, (8 * seqs, heads * HEAD_WIDTH), 0)
    head_col = lax.broadcasted_iota(jnp.int32, (8 * seqs, heads * HEAD_WIDTH), 1)
    in_group = head_row - lax.shift_left(lax.shift_right_logical(head_row, 3), 3)
    wanted = lax.shift_right_logical(head_row, 3) * QUERY_PER_KEY + in_group
    member = (in_group < QUERY_PER_KEY) & (wanted == lax.shift_right_logical(head_col, 6))
    selector = jnp.where(member, 1.0, 0.0).astype(BF16)
    product = do_in[0].astype(F32) * o_in[0].astype(F32)
    product_high = product.astype(BF16)
    product_low = (product - product_high.astype(F32)).astype(BF16)
    delta_send[...] = dot(selector, product_high, ((1,), (1,))) + dot(selector, product_low, ((1,), (1,)))
    v_got[own_rows, :] = v_send[seq]

    @pl.when(unit == 0)
    def _():
        do_got[0, :, unit_rows, :] = do_send[seq]
        delta[0, unit_piece] = delta_send[pl.ds(pl.multiple_of(seq * 8, 8), 8), :]

    def from_everyone(copies):
        for k in range(1, seqs):
            copies(k).wait_recv()

        @pl.when(unit != 0)
        def _():
            copies(0).wait_recv()

    from_everyone(q_copy)

    def halves(x):
        return jnp.concatenate([x[0:HEAD_WIDTH], x[HEAD_WIDTH:]], axis=1)

    @pl.loop(0, 2)
    def _(u):
        for h in range(QUERY_PER_KEY):
            cols = pl.ds(h * TILE, TILE)
            turned = halves(q_got[u, h].astype(F32).T).astype(BF16)
            nothing = jnp.zeros((HEAD_WIDTH, TILE), BF16)
            lt[u, 0:64, cols] = turned
            lt[u, 64:128, cols] = nothing
            lt[u, 128:192, cols] = turned
            lt[u, 192:256, cols] = nothing
        dq_acc[u] = jnp.zeros((rows, LANES), F32)
        stat_m[u] = jnp.full((8, rows), NEG_LARGE, F32)
        stat_l[u] = jnp.zeros((8, rows), F32)

    aux_row = lax.broadcasted_iota(jnp.int32, (HEAD_WIDTH, TILE), 0)
    aux_s = jnp.where(aux_row < 3, -1.0, 0.0)
    aux_v = jnp.where((aux_row >= 3) & (aux_row < 6), -1.0, 0.0)

    def packed_tile(got, t):
        return got[pl.ds(pl.multiple_of(t * HALF, HALF), HALF), :].astype(F32)

    def prepare_keys(t):
        at = pl.ds(pl.multiple_of(t * TILE, TILE), TILE)
        raw = packed_tile(k_got, t)
        zero = jnp.zeros((HALF, LANES), F32)
        mask = lax.broadcasted_iota(jnp.int32, (HALF, LANES), 1) < HEAD_WIDTH

        def spread(x):
            return jnp.concatenate([jnp.where(mask, x, zero), jnp.where(mask, pltpu.roll(x, HEAD_WIDTH, 1), zero)], axis=0)

        scaled = raw * BASE2_SCALE
        high = scaled.astype(BF16).astype(F32)
        within = pl.ds(pl.multiple_of(lax.rem(t, 2) * TILE, TILE), TILE)
        ks[within, 0:128] = spread(high).astype(BF16)
        ks[within, 128:256] = spread(scaled - high).astype(BF16)
        nothing = jnp.zeros((HEAD_WIDTH, TILE), F32)
        turned = halves(raw.T)
        k_rows[at, :] = spread(raw).astype(BF16)
        scaled = turned * BASE2_SCALE
        high = scaled.astype(BF16).astype(F32)
        ks_t[0:128, at] = jnp.concatenate([high, nothing], axis=0).astype(BF16)
        ks_t[128:256, at] = jnp.concatenate([scaled - high, aux_s], axis=0).astype(BF16)

    def prepare_values(t):
        at = pl.ds(pl.multiple_of(t * TILE, TILE), TILE)
        nothing = jnp.zeros((HEAD_WIDTH, TILE), F32)
        vs_t[0:128, at] = jnp.concatenate([nothing, halves(packed_tile(v_got, t).T)], axis=0).astype(BF16)
        vs_t[128:256, at] = jnp.concatenate([nothing, aux_v], axis=0).astype(BF16)

    def place(axis):
        r = lax.broadcasted_iota(jnp.int32, (TILE, TILE), axis)
        quarter = lax.shift_right_logical(r & (HALF - 1), 6)
        return quarter * 128 + lax.shift_right_logical(r, 8) * 64 + (r & 63)

    def stats(u, t, masked):
        w = ks[pl.ds(pl.multiple_of(lax.rem(t, 2) * TILE, TILE), TILE), :]
        news = []

        def scores(h):
            cols = pl.ds(h * TILE, TILE)
            s = dot(w, lt[u, :, cols], ((1,), (0,)))
            if masked:
                s = jnp.where(place(0) <= place(1), s, NEG_LARGE)
            top = jnp.full((8, TILE), NEG_LARGE, F32)
            for r in range(0, TILE, STRIP):
                strip = s[r : r + STRIP]
                s_buf[h, r : r + STRIP, :] = strip
                for i in range(0, STRIP, 8):
                    top = jnp.maximum(top, strip[i : i + 8])
            news.append(jnp.maximum(stat_m[u, 0:1, cols], jnp.max(top, axis=0, keepdims=True)))

        def sums(h):
            cols = pl.ds(h * TILE, TILE)
            new = jnp.broadcast_to(news[h], (8, TILE))
            total = stat_l[u, :, cols] * jnp.exp2(stat_m[u, :, cols] - new)
            for r in range(0, TILE, 8):
                total = total + jnp.exp2(s_buf[h, r : r + 8, :] - new)
            stat_l[u, :, cols] = total
            stat_m[u, :, cols] = new

        scores(0)
        for h in range(1, QUERY_PER_KEY):
            scores(h)
            sums(h - 1)
        sums(QUERY_PER_KEY - 1)

    def visit(block, step):
        @pl.loop(0, 4)
        def _(i):
            u = lax.rem(i, 2)
            t = block * 2 + lax.div(i, 2)
            last = jnp.where(u == 0, 2 * own, key_tiles - 1 - 2 * own)

            @pl.when(t < last)
            def _():
                step(u, t, False)

            @pl.when(t == last)
            def _():
                step(u, t, True)

    def cast_wait(k, got, send, receive):
        at = pl.ds(pl.multiple_of(shifted(k, -1) * (block_len // 2), block_len // 2), block_len // 2)
        remote(got.at[at], got.at[at], send.at[k], receive.at[k], shifted(k, 1), seq).wait_recv()

    @pl.loop(0, spans)
    def _(k):
        block = shifted(k, -1)

        @pl.when(needs(own, block))
        def _():
            @pl.when(k > 0)
            def _():
                cast_wait(k, k_got, kcast_ss, kcast_rs)

            prepare_keys(2 * block)
            prepare_keys(2 * block + 1)
            visit(block, stats)

        @pl.when(k == 0)
        def _():
            for copy in (v_copy, do_copy, delta_copy):
                for i in range(1, seqs):
                    copy(i).start()

            @pl.when(unit != 0)
            def _():
                do_copy(0).start()
                delta_copy(0).start()

        @pl.when(k == VALUES_AT)
        def _():
            for i in range(1, seqs):
                v_copy(i).wait_recv()
            cast_all(v_cast)

    from_everyone(delta_copy)
    from_everyone(do_copy)
    row = lax.broadcasted_iota(jnp.int32, (16, TILE), 0)

    @pl.loop(0, 2)
    def _(u):
        for h in range(QUERY_PER_KEY):
            cols = pl.ds(h * TILE, TILE)
            total = jnp.sum(stat_l[u, :, cols], axis=0, keepdims=True)
            lse = stat_m[u, 0:1, cols] + jnp.log2(total)
            pieces = [delta[u, i, h : h + 1, :] for i in range(half)]
            shifts = jnp.concatenate([x[:, :packed] for x in pieces] + [x[:, packed:] for x in pieces], axis=1)
            parts = three_parts(lse) + three_parts(shifts)
            block = jnp.zeros((16, TILE), F32)
            for i, part in enumerate(parts):
                block = jnp.where(row == i, part, block)
            lt[u, 192:208, cols] = block.astype(BF16)
            lt[u, 64:128, cols] = halves(do_got[u, h].astype(F32).T).astype(BF16)
            l1[u, h, :HALF, :], l1[u, h, HALF:, :] = paired(q_got[u, h].astype(F32), do_got[u, h].astype(F32))
            l2[u, h] = lt[u, 128:256, cols].astype(F32).T.astype(BF16)

    def main(u, t, masked):
        at = pl.ds(pl.multiple_of(t * TILE, TILE), TILE)
        within = pl.ds(pl.multiple_of(lax.rem(t, 2) * TILE, TILE), TILE)
        kw = ks_t[:, at]
        vw = vs_t[:, at]
        kr = k_rows[at, :]

        def products(h):
            lhs = jnp.concatenate([l1[u, h], l2[u, h]], axis=1)
            return dot(lhs, kw, ((1,), (0,))), dot(lhs, vw, ((1,), (0,)))

        def weights(h, s, dp):
            for r in range(0, TILE, STRIP):
                here = pl.ds(h * TILE + r, STRIP)
                p = jnp.exp2(s[r : r + STRIP])
                if masked:
                    p = jnp.where(place(1)[r : r + STRIP] <= place(0)[r : r + STRIP], p, 0.0)
                p_buf[here, :] = p.astype(BF16)
                ds_buf[here, :] = (p * dp[r : r + STRIP]).astype(BF16)

        for h in range(QUERY_PER_KEY):
            weights(h, *products(h))
            here = pl.ds(h * TILE, TILE)
            dq_acc[u, here, :] += dot(ds_buf[here, :], kr, ((1,), (0,)))
        dkv_acc[0:64, within] += dot(lt[u, 0:64, :], ds_buf[...], ((1,), (0,)))
        dkv_acc[64:128, within] += dot(lt[u, 64:128, :], p_buf[...], ((1,), (0,)))

    def part_copy(k):
        return remote(part_send.at[k], part_recv.at[k], part_ss.at[k], part_rs.at[k], shifted(k, -1), seq)

    def dq_copy(j):
        u, i = j // half, j % half
        at_span = own if u == 0 else mirror
        at = pl.ds(i * packed, packed)
        return remote(dq_send.at[u, :, at, :], dq_recv.at[seq], dq_ss.at[j], dq_rs.at[seq], at_span, j)

    def dq_arrival(g):
        return remote(dq_send.at[0, :, pl.ds(0, packed), :], dq_recv.at[g], dq_ss.at[0], dq_rs.at[g], own, g)

    def dq_pack(u):
        mask = lax.broadcasted_iota(jnp.int32, (HALF, LANES), 1) < HEAD_WIDTH
        for h in range(QUERY_PER_KEY):
            first = dq_acc[u, h * TILE : h * TILE + HALF, :]
            second = dq_acc[u, h * TILE + HALF : (h + 1) * TILE, :]
            dq_send[u, h] = (jnp.where(mask, first, pltpu.roll(second, HEAD_WIDTH, 1)) * SCORE_SCALE).astype(BF16)

    last_second = 0 * own
    for k in range(1, spans):
        last_second = jnp.where(shifted(k, -1) <= mirror, k, last_second)
    last_second = jnp.where(own <= mirror, spans, last_second)

    @pl.loop(1, spans + 1)
    def _(j):
        k = lax.rem(j, spans)
        block = shifted(k, -1)

        @pl.when(needs(own, block))
        def _():
            @pl.when(k > 0)
            def _():
                cast_wait(k, v_got, vcast_ss, vcast_rs)

            prepare_values(2 * block)
            prepare_values(2 * block + 1)
            dkv_acc[...] = jnp.zeros((LANES, block_len), F32)
            visit(block, main)
            dkv_acc[0:64, :] = dkv_acc[0:64, :] * SCORE_SCALE

            @pl.when(k > 0)
            def _():
                part_send[k] = dkv_acc[...].astype(BF16)
                part_copy(k).start()

        @pl.when(j == last_second)
        def _():
            dq_pack(1)
            for i in range(half, seqs):
                dq_copy(i).start()

    dq_pack(0)
    for j in range(half):
        @pl.when(seq == j)
        def _():
            dq_recv[j] = dq_send[0, :, j * packed : (j + 1) * packed, :]

        @pl.when(seq != j)
        def _():
            dq_copy(j).start()

    @pl.loop(1, spans)
    def _(k):
        @pl.when(needs(shifted(k, 1), own))
        def _():
            part_copy(k).wait_recv()
            dkv_acc[...] += part_recv[k].astype(F32)

    def grad_copy(k):
        there = seq_shifted(k, 1)
        return remote(grad_send.at[there], grad_recv.at[k], grad_ss.at[k], grad_rs.at[k], own, there)

    for j in range(seqs // half):
        turned = dkv_acc[:, j * TILE : (j + 1) * TILE].T
        for i in range(half):
            at = i * packed
            piece = jnp.concatenate([turned[at : at + packed], turned[at + HALF : at + HALF + packed]], axis=0)
            grad_send[j * half + i] = piece.astype(BF16)
    for k in range(1, seqs):
        grad_copy(k).start()
    grad_recv[0] = grad_send[seq]

    for g in range(seqs):
        remote_here = jnp.logical_or(unit != 0, seq != g)

        @pl.when(remote_here)
        def _():
            dq_arrival(g).wait_recv()

    for i in range(heads // 2):
        a, b = (dq_recv[n // QUERY_PER_KEY, n % QUERY_PER_KEY].astype(F32) for n in (2 * i, 2 * i + 1))
        at = slice(i * LANES, (i + 1) * LANES)
        qg_out[0, :packed, at], qg_out[0, packed:, at] = paired(a, b)

    for k in range(1, seqs):
        grad_copy(k).wait_recv()
    for i in range(seqs // 2):
        a = grad_recv[lax.rem(seq + seqs - 2 * i, seqs)]
        b = grad_recv[lax.rem(seq + seqs - 2 * i - 1, seqs)]
        key_part, value_part = paired(a.astype(F32), b.astype(F32))
        kg_out[0, :, i * LANES : (i + 1) * LANES] = key_part
        vg_out[0, :, i * LANES : (i + 1) * LANES] = value_part

    for k in range(1, seqs):
        for copy in (k_copy, v_copy, q_copy, do_copy, delta_copy, grad_copy):
            copy(k).wait_send()

    @pl.when(unit != 0)
    def _():
        for copy in (q_copy, do_copy, delta_copy):
            copy(0).wait_send()

    for j in range(seqs):
        if j < half:
            @pl.when(seq != j)
            def _():
                dq_copy(j).wait_send()
        else:
            dq_copy(j).wait_send()

    @pl.loop(1, spans)
    def _(k):
        @pl.when(needs(shifted(k, 1), own))
        def _():
            k_cast(k).wait_send()
            v_cast(k).wait_send()

        @pl.when(needs(own, shifted(k, -1)))
        def _():
            part_copy(k).wait_send()


def solution(mesh):
    seqs, spans = mesh.shape["seq"], mesh.shape["span"]
    spec = P("span", "seq", None)

    def per_device(queries, keys, values, attn_output, out_grad):
        tokens = queries.shape[1]
        block_len = tokens * seqs
        total = block_len * spans
        rows = QUERY_PER_KEY * TILE
        vmem = pl.BlockSpec(memory_space=pltpu.VMEM)
        dma = pltpu.SemaphoreType.DMA
        return pl.pallas_call(
            functools.partial(fused_kernel, seqs, spans),
            out_shape=(
                jax.ShapeDtypeStruct(queries.shape, BF16),
                jax.ShapeDtypeStruct(keys.shape, BF16),
                jax.ShapeDtypeStruct(values.shape, BF16),
            ),
            in_specs=[vmem] * 5,
            out_specs=(vmem,) * 3,
            scratch_shapes=[
                pltpu.VMEM((total // 2, LANES), BF16),
                pltpu.VMEM((total // 2, LANES), BF16),
                pltpu.VMEM((2, QUERY_PER_KEY, HALF, LANES), BF16),
                pltpu.VMEM((2, QUERY_PER_KEY, HALF, LANES), BF16),
                pltpu.VMEM((2, seqs // 2, 8, tokens), F32),
                pltpu.VMEM((2, 256, rows), BF16),
                pltpu.VMEM((2, QUERY_PER_KEY, TILE, LANES), BF16),
                pltpu.VMEM((2, QUERY_PER_KEY, TILE, LANES), BF16),
                pltpu.VMEM((total, LANES), BF16),
                pltpu.VMEM((256, total), BF16),
                pltpu.VMEM((256, total), BF16),
                pltpu.VMEM((2 * TILE, 256), BF16),
                pltpu.VMEM((QUERY_PER_KEY, TILE, TILE), F32),
                pltpu.VMEM((2, 8, rows), F32),
                pltpu.VMEM((2, 8, rows), F32),
                pltpu.VMEM((2, rows, LANES), F32),
                pltpu.VMEM((rows, TILE), BF16),
                pltpu.VMEM((rows, TILE), BF16),
                pltpu.VMEM((LANES, block_len), F32),
                pltpu.VMEM((seqs, tokens // 2, LANES), BF16),
                pltpu.VMEM((seqs, tokens // 2, LANES), BF16),
                pltpu.VMEM((seqs, QUERY_PER_KEY, tokens // 2, LANES), BF16),
                pltpu.VMEM((seqs, QUERY_PER_KEY, tokens // 2, LANES), BF16),
                pltpu.VMEM((8 * seqs, tokens), F32),
                pltpu.VMEM((spans, LANES, block_len), BF16),
                pltpu.VMEM((spans, LANES, block_len), BF16),
                pltpu.VMEM((2, QUERY_PER_KEY, HALF, LANES), BF16),
                pltpu.VMEM((seqs, QUERY_PER_KEY, tokens // 2, LANES), BF16),
                pltpu.VMEM((seqs, tokens, LANES), BF16),
                pltpu.VMEM((seqs, tokens, LANES), BF16),
            ]
            + [dma((seqs,))] * 10 + [dma((spans,))] * 6 + [dma((seqs,))] * 4,
            compiler_params=pltpu.CompilerParams(
                vmem_limit_bytes=60 * 1024 * 1024, collective_id=0, has_side_effects=True
            ),
            name="attention_grads",
        )(queries, keys, values, attn_output, out_grad)

    return jax.shard_map(
        per_device, mesh=mesh, in_specs=(spec,) * 5, out_specs=(spec,) * 3, check_vma=False
    )
```
